128 devices in a mesh: pole: 16 (over y, z_lo, core), row: 2 (over z_hi), col: 4 (over x).
Axes of the slice: x: 4, y: 4, z: 4 (z_hi: 2, z_lo: 2; z = z_hi * 2 + z_lo), core: 2. Of those that a mesh axis runs over, the one named last changes fastest.
Arguments:
- l_factor: float32 [16, 2, 6, 512, 6, 512], P('pole', None, None, 'row', None, 'col'), may hold values from -0.21875 to 0.21875
- dinv: float32 [16, 2, 6, 512, 512], P('pole', None, None, 'row', 'col'), may hold values from -8 to 8, as said below
- weights: float32 [16, 2], P('pole'), may hold values from -4 to 4
- tiles: int32 [6, 24], replicated, may hold values 0 or 1
Outputs:
- density: float32 [6, 2, 256, 6, 512], P(None, 'row', 'pole', None, 'col')
The draws below stay inside these ranges and needn't reach their ends.
Inputs may be any that keep to these rules, and one draw needn't show every extreme that they name: Each of dinv's blocks is a symmetric complex matrix.
All inputs are finite; a program needn't handle non-finite values.
Results may differ from the reference program's by a relative error of at most 0.00012.
Values sent between devices are 32-bit elements; how exact they have to be, the bound alone decides.
A program may use at most 192 MiB of HBM per device.

```python
import jax
import jax.numpy as jnp
from jax import lax

W = 512
NS = 6
TILE = 128
POLES = 16
N_ROW = 2


def draw_dinv(key, part):
    first, second, third = jax.random.split(jax.random.fold_in(key, 17), 3)
    noise = jax.random.normal(first, (POLES, 2, NS, W, W), jnp.float32)
    sym = (noise + jnp.swapaxes(noise, 3, 4)) * (0.6 / (2.0 * W) ** 0.5)
    real_diag = jax.random.uniform(second, (POLES, NS, W), jnp.float32, 0.5, 1.5)
    imag_diag = jax.random.uniform(third, (POLES, NS, W), jnp.float32, -0.5, 0.5)
    eye = jnp.eye(W, dtype=jnp.float32)
    diag = jnp.stack([real_diag, imag_diag], axis=1)[..., None] * eye
    result = sym + diag
    return jnp.clip(result, -8.0, 8.0)


def touch_ends(values, stream_key, least, high):
    longest = values.shape.index(max(values.shape))
    spots = []
    for shift in (0, 1):
        where = [jax.random.randint(jax.random.fold_in(stream_key, axis), (), 0, length) for axis, length in enumerate(values.shape)]
        where[longest] = (where[longest] + shift) % values.shape[longest]
        spots.append(tuple(where))
    return values.at[spots[0]].set(least).at[spots[1]].set(high)


def steps_of(key, shape, shards, least, largest):
    level = 1.0
    for dim, blocks in shards:
        steps = jax.random.uniform(jax.random.fold_in(jax.random.fold_in(key, 6), dim), (blocks,), jnp.float32, least / len(shards), largest / len(shards))
        level = level * jnp.repeat(jnp.exp(steps), shape[dim] // blocks).reshape((-1,) + (1,) * (len(shape) - 1 - dim))
    return level


def centred(key, shape, deviation, limit, pieces=(), held_as=jnp.bfloat16):
    values = jax.random.normal(key, shape, jnp.float32) * deviation
    if len(pieces) > 0:
        values = steps_of(key, shape, pieces, -0.22, 0.18) * values
    return jnp.clip(values, min=-limit, max=limit).astype(held_as)


def setup_inputs(seed: int = 0) -> dict:
    streams_of = jax.random.split(jax.random.key(seed), 5)
    return {
        "l_factor": centred(streams_of[0], (POLES, 2, NS, W, NS, W), (NS * W // 4) ** -0.5, 0.21875, ((0, 16), (3, 2), (5, 4)), jnp.float32),
        "dinv": draw_dinv(jax.random.fold_in(streams_of[4], 71), 0),
        "weights": centred(streams_of[2], (POLES, 2), 1.0, 4.0, ((0, 16),), jnp.float32),
        "tiles": touch_ends((jax.random.randint(streams_of[3], (NS, NS * W // TILE), 0, 4) < 3).astype(jnp.int32), jax.random.fold_in(streams_of[3], 1), 0, 1),
    }


def cdot_t(left, right):
    dims = (((0,), (0,)), ((), ()))

    def single(first, second):
        return lax.dot_general(first, second, dims, precision=lax.Precision.HIGHEST, preferred_element_type=jnp.float32)

    real = single(left[0], right[0]) - single(left[1], right[1])
    imag = single(left[0], right[1]) + single(left[1], right[0])
    return jnp.stack([real, imag])


def reference(l_factor, dinv, weights, tiles):
    total = NS * W
    row_keep = jnp.repeat(tiles, TILE, axis=1)
    keep = jnp.repeat(row_keep, W, axis=0).T.astype(jnp.float32)

    def one_pole(carry, inputs):
        factor, diag_inv, weight = inputs
        lower = factor.reshape(2, total, total) * keep[None]
        inverse = jnp.zeros((2, total, total), jnp.float32)
        last = (NS - 1) * W
        inverse = inverse.at[:, last:, last:].set(diag_inv[:, NS - 1])
        for step in range(NS - 2, -1, -1):
            start = step * W
            after = (step + 1) * W
            panel = lower[:, after:, start:start + W]
            block = inverse[:, after:, after:]
            row_part = -cdot_t(panel, block)
            inverse = inverse.at[:, start:start + W, after:].set(row_part)
            column = jnp.swapaxes(row_part, 1, 2)
            inverse = inverse.at[:, after:, start:start + W].set(column)
            inverse = inverse.at[:, start:start + W, start:start + W].set(diag_inv[:, step] - cdot_t(panel, column))
        return carry + weight[0] * inverse[0] - weight[1] * inverse[1], None

    summed, unused = lax.scan(one_pole, jnp.zeros((total, total), jnp.float32), (l_factor, dinv, weights))
    return summed.reshape(NS, N_ROW, W // N_ROW, NS, W)
```

```python
import functools

import jax
import jax.numpy as jnp
from jax import lax
from jax.experimental import pallas as pl
from jax.experimental.pallas import tpu as pltpu
from jax.sharding import Mesh
from jax.sharding import PartitionSpec as P

AXES = ("a", "b", "zl", "core", "zh", "x")
MESH = pl.DeviceIdType.MESH


def block_order(nsup):
    lower = [("L", row, col) for col in range(1, nsup - 1) for row in range(col + 1, nsup)]
    diag = [("D", col, col) for col in range(nsup - 1, 0, -1)]
    first = [("L", row, 0) for row in range(1, nsup)]
    return lower + diag + first + [("D", 0, 0)]


def gather_kernel(nb, pack, full, z_send, z_recv, x_send, x_recv, c_send, c_recv):
    zl, core, zh, x = (lax.axis_index(n) for n in ("zl", "core", "zh", "x"))
    ncol = lax.axis_size("x")
    right, left = lax.rem(x + 1, ncol), lax.rem(x + ncol - 1, ncol)
    far = lax.rem(x + 2, ncol)
    to_z = {"zl": 1 - zl, "core": zh, "zh": core}
    to_right, to_left, to_core = {"x": right}, {"x": left}, {"core": 1 - core}
    rows, cols = pack.shape[2], pack.shape[3]

    barrier = pltpu.get_barrier_semaphore()
    for peer in (to_z, to_right, to_left, to_core):
        pl.semaphore_signal(barrier, inc=1, device_id=peer, device_id_type=MESH)
    pl.semaphore_wait(barrier, 4)

    def tile(b, row, col, parts=pl.ds(0, 2)):
        return full.at[
            b,
            parts,
            pl.ds(pl.multiple_of(row * rows, rows), rows),
            pl.ds(pl.multiple_of(col * cols, cols), cols),
        ]

    def z_copy(b):
        return pltpu.make_async_remote_copy(
            pack.at[b], tile(b, zh, x), z_send.at[b], z_recv.at[b], device_id=to_z, device_id_type=MESH
        )

    def z_wait(b):
        pltpu.make_async_remote_copy(
            pack.at[b], tile(b, core, x), z_send.at[b], z_recv.at[b], device_id=to_z, device_id_type=MESH
        ).wait_recv()

    half = (pl.ds(0, 1), pl.ds(1, 1))

    def x_copy(b, kind, col, parts, peer):
        ref = tile(b, core, col, parts)
        return pltpu.make_async_remote_copy(
            ref, ref, x_send.at[kind, b], x_recv.at[kind, b], device_id=peer, device_id_type=MESH
        )

    def c_copy(b, kind, col, parts=pl.ds(0, 2), row=None):
        ref = tile(b, core if row is None else row, col, parts)
        return pltpu.make_async_remote_copy(
            ref, ref, c_send.at[kind, b], c_recv.at[kind, b], device_id=to_core, device_id_type=MESH
        )

    both = pl.ds(0, 2)
    last = nb - 1

    @pl.loop(0, nb)
    def _(b):
        z_copy(b).start()

    def own(b):
        z_wait(b)
        x_copy(b, 0, x, both, to_right).start()
        x_copy(b, 1, x, both, to_left).start()
        c_copy(b, 0, x).start()

    def pass_on(b):
        x_copy(b, 0, left, both, to_right).wait_recv()
        x_copy(b, 2, left, half[0], to_right).start()
        c_copy(b, 1, left).start()
        x_copy(b, 1, right, both, to_left).wait_recv()
        x_copy(b, 3, right, half[1], to_left).start()
        c_copy(b, 2, right).start()

    def finish(b):
        x_copy(b, 2, far, half[0], to_right).wait_recv()
        c_copy(b, 3, far, half[0]).start()
        x_copy(b, 3, far, half[1], to_left).wait_recv()
        c_copy(b, 4, far, half[1]).start()

    own(0)
    own(1)
    pass_on(0)

    @pl.loop(2, last)
    def _(b):
        own(b)
        pass_on(b - 1)
        finish(b - 2)

    pass_on(last - 1)
    z_wait(last)
    c_copy(last, 0, x).start()
    finish(last - 2)
    finish(last - 1)

    @pl.loop(0, last)
    def _(b):
        z_copy(b).wait_send()
        x_copy(b, 0, x, both, to_right).wait_send()
        x_copy(b, 1, x, both, to_left).wait_send()
        x_copy(b, 2, left, half[0], to_right).wait_send()
        x_copy(b, 3, right, half[1], to_left).wait_send()
        for kind, col, parts in ((0, x, both), (1, left, both), (2, right, both), (3, far, half[0]), (4, far, half[1])):
            c_copy(b, kind, col, parts).wait_send()
            c_copy(b, kind, col, parts, 1 - core).wait_recv()

    z_copy(last).wait_send()
    c_copy(last, 0, x).wait_send()
    c_copy(last, 0, x, both, 1 - core).wait_recv()


def gather_blocks(pack, ncol):
    nb, parts, rows, cols = pack.shape
    sems = pltpu.SemaphoreType.DMA
    return pl.pallas_call(
        functools.partial(gather_kernel, nb),
        out_shape=jax.ShapeDtypeStruct((nb, parts, 2 * rows, ncol * cols), jnp.float32),
        in_specs=[pl.BlockSpec(memory_space=pl.ANY)],
        out_specs=pl.BlockSpec(memory_space=pl.ANY),
        scratch_shapes=[sems((nb,)), sems((nb,)), sems((4, nb)), sems((4, nb)), sems((5, nb)), sems((5, nb))],
        compiler_params=pltpu.CompilerParams(collective_id=0, has_side_effects=True),
    )(pack)


def product(left, right, contract):
    def single(a, b):
        return lax.dot_general(
            a, b, (((contract,), (0,)), ((), ())), precision=lax.Precision.HIGH, preferred_element_type=jnp.float32
        )

    n = right[0].shape[1]
    both = jnp.concatenate(right, axis=1)
    by_real, by_imag = single(left[0], both), single(left[1], both)
    return by_real[:, :n] - by_imag[:, n:], by_real[:, n:] + by_imag[:, :n]


def minus(first, second):
    return first[0] - second[0], first[1] - second[1]


def on_device(l_factor, dinv, weights, tiles):
    zl, core, zh, x = (lax.axis_index(n) for n in ("zl", "core", "zh", "x"))
    ncol = lax.axis_size("x")
    factor, diag_inv = l_factor[0], dinv[0]
    nsup, rows, cols = factor.shape[1], factor.shape[2], factor.shape[4]
    width = 2 * rows
    tile_rows = nsup * width // tiles.shape[1]
    expanded = jnp.repeat(tiles.reshape(nsup, nsup, -1), tile_rows, axis=2)
    keep = lax.dynamic_slice_in_dim(expanded, zh * rows, rows, 2).astype(jnp.float32)

    order = block_order(nsup)
    where = {item: i for i, item in enumerate(order)}
    pack = jnp.stack(
        [
            factor[:, row, :, col, :] * keep[col, row][None, :, None] if kind == "L" else diag_inv[:, row]
            for kind, row, col in order
        ]
    )
    perm = [
        ((l * 2 + k) * 2 + h, ((1 - l) * 2 + h) * 2 + k) for l in range(2) for k in range(2) for h in range(2)
    ]
    weight = lax.ppermute(weights[0], ("zl", "core", "zh"), perm)
    full = gather_blocks(pack, ncol)

    n = cols // 2
    start = x * cols + core * n

    def block(kind, row, col):
        both = full[where[(kind, row, col)]]
        return both[0], both[1]

    def mine(kind, row, col):
        both = lax.dynamic_slice_in_dim(full[where[(kind, row, col)]], start, n, 2)
        return both[0], both[1]

    z = {}
    for row in range(1, nsup):
        pieces = [mine("L", row, col) for col in range(row)]
        total = tuple(jnp.concatenate([p[i] for p in pieces], axis=1) for i in range(2))
        for mid in range(1, row):
            term = product(block("L", row, mid), z[mid], 1)
            total = tuple(
                jnp.concatenate([t[:, : mid * n] - m, t[:, mid * n :]], axis=1) for t, m in zip(total, term)
            )
        z[row] = total
    h = {}
    for row in range(nsup - 1, -1, -1):
        own = mine("D", row, row)
        if row > 0:
            t = product(block("D", row, row), z[row], 1)
            own = tuple(jnp.concatenate([-t[i], own[i]], axis=1) for i in range(2))
        if row < nsup - 1:
            left = tuple(
                jnp.concatenate([block("L", low, row)[i] for low in range(row + 1, nsup)], axis=0) for i in range(2)
            )
            right = tuple(
                jnp.concatenate([h[low][i][:, : (row + 1) * n] for low in range(row + 1, nsup)], axis=0)
                for i in range(2)
            )
            own = minus(own, product(left, right, 0))
        h[row] = own
    pairs = [(row, col) for row in range(nsup) for col in range(row + 1)]
    partial_sum = jnp.concatenate([weight[0] * h[row][0] - weight[1] * h[row][1] for row in range(nsup)], axis=1)
    share = lax.psum_scatter(partial_sum, ("zh", "a", "b", "zl"), scatter_dimension=0, tiled=True)
    share = share.reshape(share.shape[0], len(pairs), n)

    low = lax.all_to_all(share, "core", split_axis=0, concat_axis=2, tiled=True)
    off = jnp.stack([share[:, i] for i, (row, col) in enumerate(pairs) if row > col], axis=0)
    swapped = lax.all_to_all(off, ("b", "zl"), split_axis=2, concat_axis=1, tiled=True)
    sizes = [lax.axis_size(name) for name in AXES]
    jumps = []
    for a in range(2):
        for b in range(2):
            for l in range(2):
                for k in range(2):
                    for h_ in range(2):
                        for c in range(ncol):
                            src = ((((a * 2 + b) * 2 + l) * 2 + k) * 2 + h_) * ncol + c
                            d = (c % 2, k, b, l, c // 2, h_ * 2 + a)
                            dst = ((((d[0] * 2 + d[1]) * 2 + d[2]) * 2 + d[3]) * 2 + d[4]) * ncol + d[5]
                            jumps.append((src, dst))
    mirrored = jnp.swapaxes(lax.ppermute(swapped, AXES, jumps), 1, 2)

    spot = {pair: i for i, pair in enumerate(pairs)}
    offs = {pair: i for i, pair in enumerate(p for p in pairs if p[0] > p[1])}
    grid = [
        jnp.stack([low[:, spot[(row, col)]] if row >= col else mirrored[offs[(col, row)]] for col in range(nsup)], axis=1)
        for row in range(nsup)
    ]
    return jnp.stack(grid)[:, None]


def solution(mesh):
    fine = Mesh(mesh.devices.reshape(2, 2, 2, 2, 2, 4), AXES)
    pole = ("a", "b", "zl", "core")
    return jax.shard_map(
        on_device,
        mesh=fine,
        in_specs=(P(pole, None, None, "zh", None, "x"), P(pole, None, None, "zh", "x"), P(pole, None), P()),
        out_specs=P(None, "zh", pole, None, "x"),
        check_vma=False,
    )
```

```python
import functools

import jax
import jax.numpy as jnp
from jax import lax
from jax.experimental import pallas as pl
from jax.experimental.pallas import tpu as pltpu
from jax.sharding import Mesh
from jax.sharding import PartitionSpec as P

AXES = ("a", "b", "zl", "core", "zh", "x")
MESH = pl.DeviceIdType.MESH


def block_order(nsup):
    lower = [("L", row, col) for col in range(1, nsup - 1) for row in range(col + 1, nsup)]
    diag = [("D", col, col) for col in range(nsup - 1, 0, -1)]
    first = [("L", row, 0) for row in range(1, nsup)]
    return lower + diag + first + [("D", 0, 0)]


def tri(row):
    return row * (row + 1) // 2


def split(value):
    high = value.astype(jnp.bfloat16)
    return high, (value - high.astype(jnp.float32)).astype(jnp.bfloat16)


def dot(a, b, dim):
    return lax.dot_general(a, b, (((1,), (dim,)), ((), ())), preferred_element_type=jnp.float32)


def window_kernel(
    nsup, pack, weight, full, out,
    blk, own_cols, flip, acc_z, acc_g, z_high, z_low, g_high, g_low, real, part1, sum1, part2,
    z_send, z_recv, x_send, x_recv, c_send, c_recv, r_send, r_recv, blk_sem, own_sem,
):
    order = block_order(nsup)
    where = {item: i for i, item in enumerate(order)}
    nb = len(order)
    last = nb - 1
    first0 = where[("L", 1, 0)]
    a_, b_, zl, core, zh, x = (lax.axis_index(n) for n in AXES)
    ncol = lax.axis_size("x")
    rows, cols = pack.shape[2], pack.shape[3]
    width = full.shape[2]
    half_w = width // 2
    n = cols // 2
    unit = 2 * n
    right, left, far = lax.rem(x + 1, ncol), lax.rem(x + ncol - 1, ncol), lax.rem(x + 2, ncol)
    to_z = {"zl": 1 - zl, "core": zh, "zh": core}
    to_right, to_left, to_core = {"x": right}, {"x": left}, {"core": 1 - core}

    def other(value, flag):
        return 1 - value if flag else value

    z_peers = [(other(zh, d >> 1), other(zl, d & 1)) for d in (1, 2, 3)]
    y_peers = [(other(a_, d >> 1), other(b_, d & 1)) for d in (1, 2, 3)]
    barrier = pltpu.get_barrier_semaphore()
    peers = [to_z, to_right, to_left, to_core]
    peers += [{"zh": h, "zl": l} for h, l in z_peers] + [{"a": p, "b": q} for p, q in y_peers]
    for peer in peers:
        pl.semaphore_signal(barrier, inc=1, device_id=peer, device_id_type=MESH)
    pl.semaphore_wait(barrier, len(peers))

    both, half0, half1 = pl.ds(0, 2), pl.ds(0, 1), pl.ds(1, 1)

    def tile(b, row, col, parts=both):
        return full.at[
            b,
            parts,
            pl.ds(pl.multiple_of(row * rows, rows), rows),
            pl.ds(pl.multiple_of(col * cols, cols), cols),
        ]

    def remote(src, dst, send, recv, peer):
        return pltpu.make_async_remote_copy(src, dst, send, recv, device_id=peer, device_id_type=MESH)

    def z_copy(b, row):
        return remote(pack.at[b], tile(b, row, x), z_send.at[b], z_recv.at[b], to_z)

    def x_copy(b, kind, col, parts, peer):
        ref = tile(b, core, col, parts)
        return remote(ref, ref, x_send.at[kind, b], x_recv.at[kind, b], peer)

    def c_copy(b, kind, col, parts, row):
        ref = tile(b, row, col, parts)
        return remote(ref, ref, c_send.at[kind, b], c_recv.at[kind, b], to_core)

    c_kinds = ((0, x, both), (1, left, both), (2, right, both), (3, far, half0), (4, far, half1))

    z_order, late = [0, 1], list(range(first0, nb))
    for b in range(2, first0):
        z_order.append(b)
        if late:
            z_order.append(late.pop(0))
    z_order += late
    for b in z_order:
        z_copy(b, zh).start()

    def own_part(b):
        z_copy(b, core).wait_recv()
        c_copy(b, 0, x, both, core).start()

    def own(b):
        if b < first0:
            own_part(b)
        x_copy(b, 0, x, both, to_right).start()
        x_copy(b, 1, x, both, to_left).start()

    def pass_on(b):
        x_copy(b, 0, left, both, to_right).wait_recv()
        x_copy(b, 2, left, half0, to_right).start()
        c_copy(b, 1, left, both, core).start()
        x_copy(b, 1, right, both, to_left).wait_recv()
        x_copy(b, 3, right, half1, to_left).start()
        c_copy(b, 2, right, both, core).start()

    def finish(b):
        x_copy(b, 2, far, half0, to_right).wait_recv()
        c_copy(b, 3, far, half0, core).start()
        x_copy(b, 3, far, half1, to_left).wait_recv()
        c_copy(b, 4, far, half1, core).start()

    def service(s):
        if s + 2 < last:
            own(s + 2)
        if 1 <= s and first0 + s - 1 <= last:
            own_part(first0 + s - 1)
        if s < last:
            pass_on(s)
        if 1 <= s <= last:
            finish(s - 1)

    def arrived(b):
        for kind, col, parts in c_kinds:
            if kind > 0 or b < first0:
                c_copy(b, kind, col, parts, 1 - core).wait_recv()

    def blk_copy(b, slot):
        return pltpu.make_async_copy(full.at[b], blk.at[slot], blk_sem.at[slot])

    def unit_rows(index):
        return pl.ds(pl.multiple_of(index * unit, unit), unit)

    def turned(q):
        flip[q] = jnp.transpose(own_cols[q])
        return flip[q, pl.ds(pl.multiple_of(core * n, n), n), :]

    def load_own(b):
        copy = pltpu.make_async_copy(
            full.at[b, :, :, pl.ds(pl.multiple_of(x * cols, cols), cols)], own_cols, own_sem
        )
        copy.start()
        copy.wait()

    def set_first(acc, index):
        for q in range(2):
            acc[0, pl.ds(index * unit + q * n, n), :] = turned(q)
        acc[1, pl.ds(index * unit, unit), :] = jnp.zeros((unit, width), jnp.float32)

    def begin():
        for row in range(1, nsup):
            c_copy(first0 + row - 1, 0, x, both, 1 - core).wait_recv()
            load_own(first0 + row - 1)
            set_first(acc_z, tri(row - 1))
        finish_z(1)

    def joined(acc, index):
        p, q = acc[0, unit_rows(index), :], acc[1, unit_rows(index), :]
        return p[:n] - q[n:], p[n:] + q[:n]

    def finish_z(row):
        @pl.loop(0, row)
        def _(k):
            re, im = joined(acc_z, tri(row - 1) + k)
            high, low = split(-jnp.concatenate([re, im], axis=0))
            z_high[unit_rows(tri(row) + k), :] = high
            z_low[unit_rows(tri(row) + k), :] = low

        lane = lax.broadcasted_iota(jnp.int32, (unit, width), 1)
        line = lax.broadcasted_iota(jnp.int32, (unit, width), 0)
        hit = (lane == line + x * cols + core * n) & (line < n)
        z_high[pl.ds((tri(row) + row) * unit, unit), :] = jnp.where(hit, 1.0, 0.0).astype(jnp.bfloat16)
        z_low[pl.ds((tri(row) + row) * unit, unit), :] = jnp.zeros((unit, width), jnp.bfloat16)

    def multiply(acc, acc_at, high, low, at, units, slot, transposed, fresh):
        m = units * unit
        here, there = pl.ds(at * unit, m), pl.ds(acc_at * unit, m)

        @pl.loop(0, 4)
        def _(i):
            q, piece = i // 2, pl.ds(pl.multiple_of((i % 2) * half_w, half_w), half_w)
            if transposed:
                right_high, right_low = split(blk[slot, q, piece, :])
                dim = 1
            else:
                right_high, right_low = split(blk[slot, q, :, piece])
                dim = 0
            total = dot(high[here, :], right_high, dim)
            total += dot(low[here, :], right_high, dim)
            total += dot(high[here, :], right_low, dim)
            if fresh:
                acc[q, there, piece] = total
            else:
                acc[q, there, piece] += total

    def forward(row, mid, slot):
        own_cols[...] = blk[slot, :, :, pl.ds(pl.multiple_of(x * cols, cols), cols)]
        set_first(acc_z, tri(row - 1) + mid)
        multiply(acc_z, tri(row - 1), z_high, z_low, tri(mid), mid, slot, True, False)
        if row == nsup - 1:
            finish_z(mid + 1)

    def backward(row, low_row, slot):
        if low_row == row:
            multiply(acc_g, 0, z_high, z_low, tri(row), row + 1, slot, False, True)
        else:
            multiply(acc_g, 0, g_high, g_low, tri(low_row), row + 1, slot, False, False)
        if low_row == nsup - 1:
            finish_g(row)

    def finish_g(row):
        w_re, w_im = weight[0], weight[1]

        @pl.loop(0, row + 1)
        def _(k):
            re, im = joined(acc_g, k)
            real[tri(row) + k] = (w_re * re - w_im * im).reshape(real.shape[1:])
            if row > 0:
                high, low = split(-jnp.concatenate([re, im], axis=0))
                g_high[unit_rows(tri(row) + k), :] = high
                g_low[unit_rows(tri(row) + k), :] = low

        for copy in first_stage(row):
            copy.start()

    def first_stage(row):
        span = pl.ds(tri(row), row + 1)
        copies = []
        for d, (h, l) in enumerate(z_peers):
            lanes = pl.ds(pl.multiple_of(h * half_w, half_w), half_w)
            copies.append(
                remote(
                    real.at[span, :, l, :, lanes], part1.at[d, span], r_send.at[0, row, d], r_recv.at[0, row, d],
                    {"zh": h, "zl": l},
                )
            )
        return copies

    def second_stage(row):
        span = pl.ds(tri(row), row + 1)
        copies = []
        for d, (p, q) in enumerate(y_peers):
            lanes = pl.ds(pl.multiple_of(p * cols, cols), cols)
            copies.append(
                remote(
                    sum1.at[span, q, :, lanes], part2.at[d, span], r_send.at[1, row, d], r_recv.at[1, row, d],
                    {"a": p, "b": q},
                )
            )
        return copies

    def reduce_first(row):
        for copy in first_stage(row):
            copy.wait_recv()
        span = pl.ds(tri(row), row + 1)
        lanes = pl.ds(pl.multiple_of(zh * half_w, half_w), half_w)
        sum1[span] = real[span, :, zl, :, lanes] + part1[0, span] + part1[1, span] + part1[2, span]
        for copy in second_stage(row):
            copy.start()

    def reduce_second(row):
        for copy in second_stage(row):
            copy.wait_recv()
        span = pl.ds(tri(row), row + 1)
        lanes = pl.ds(pl.multiple_of(a_ * cols, cols), cols)
        out[span] = sum1[span, b_, :, lanes] + part2[0, span] + part2[1, span] + part2[2, span]

    items = []
    for b in range(nsup * (nsup - 1) // 2 - (nsup - 1)):
        kind, row, mid = order[b]
        items.append((functools.partial(forward, row, mid), b, b, mid))
    for row in range(nsup - 1, 0, -1):
        items.append((functools.partial(backward, row, row), where[("D", row, row)], where[("D", row, row)], row + 1))
        for low_row in range(row + 1, nsup):
            items.append(
                (functools.partial(backward, row, low_row), where[("L", low_row, row)], where[("D", row, row)], row + 1)
            )
    for low_row in range(1, nsup):
        b = where[("L", low_row, 0)]
        items.append((functools.partial(backward, 0, low_row), b, b, 1))

    own(0)
    own(1)
    state = {"done": -1, "loaded": -1}
    seen = set()

    def fetch(i):
        if i <= state["loaded"] or i >= len(items) or items[i][2] + 1 > state["done"]:
            return
        b = items[i][1]
        if b not in seen:
            seen.add(b)
            arrived(b)
        blk_copy(b, i % 2).start()
        state["loaded"] = i

    todo, started, summed = 0, [], []
    ready_at = first0 - where[("L", 1, 0)] + nsup + 1
    finals = {}
    for i, (fn, b, avail, units) in enumerate(items):
        if fn.func is backward and fn.args[1] == nsup - 1:
            finals[i] = fn.args[0]
    for s in range(last + 1):
        service(s)
        state["done"] = s
        if s == ready_at:
            begin()
        if s < ready_at:
            continue
        for row in summed:
            reduce_second(row)
        summed = list(started)
        for row in started:
            reduce_first(row)
        started = []
        budget = 6 if s < last else 10**6
        while todo < len(items) and items[todo][2] + 1 <= s and budget > 0:
            fetch(todo)
            fetch(todo + 1)
            blk_copy(items[todo][1], todo % 2).wait()
            if todo == len(items) - nsup + 1:
                c_copy(last, 0, x, both, 1 - core).wait_recv()
                load_own(last)
                set_first(acc_g, 0)
            items[todo][0](todo % 2)
            budget -= items[todo][3]
            if todo in finals:
                started.append(finals[todo])
            todo += 1
    for row in summed:
        reduce_second(row)
    for row in started:
        reduce_first(row)
    for row in started:
        reduce_second(row)

    for b in range(nb):
        z_copy(b, zh).wait_send()
        c_copy(b, 0, x, both, core).wait_send()
        if b < last:
            x_copy(b, 0, x, both, to_right).wait_send()
            x_copy(b, 1, x, both, to_left).wait_send()
            x_copy(b, 2, left, half0, to_right).wait_send()
            x_copy(b, 3, right, half1, to_left).wait_send()
            for kind, col, parts in c_kinds[1:]:
                c_copy(b, kind, col, parts, core).wait_send()
    for row in range(nsup):
        for copy in first_stage(row) + second_stage(row):
            copy.wait_send()


def window_share(pack, weight, nsup, ncol):
    nb, parts, rows, cols = pack.shape
    width, unit, pairs = 2 * rows, cols, tri(nsup)
    sems = pltpu.SemaphoreType.DMA
    f32, bf16 = jnp.float32, jnp.bfloat16
    return pl.pallas_call(
        functools.partial(window_kernel, nsup),
        out_shape=(
            jax.ShapeDtypeStruct((nb, parts, width, width), f32),
            jax.ShapeDtypeStruct((pairs, 16, cols), f32),
        ),
        in_specs=[pl.BlockSpec(memory_space=pl.ANY), pl.BlockSpec(memory_space=pltpu.SMEM)],
        out_specs=(pl.BlockSpec(memory_space=pl.ANY), pl.BlockSpec(memory_space=pltpu.VMEM)),
        scratch_shapes=[
            pltpu.VMEM((2, parts, width, width), f32),
            pltpu.VMEM((parts, width, cols), f32),
            pltpu.VMEM((parts, cols, width), f32),
            pltpu.VMEM((2, tri(nsup - 1) * unit, width), f32),
            pltpu.VMEM((2, nsup * unit, width), f32),
            pltpu.VMEM((pairs * unit, width), bf16),
            pltpu.VMEM((pairs * unit, width), bf16),
            pltpu.VMEM((pairs * unit, width), bf16),
            pltpu.VMEM((pairs * unit, width), bf16),
            pltpu.VMEM((pairs, 2, 2, 16, width), f32),
            pltpu.VMEM((3, pairs, 2, 16, width // 2), f32),
            pltpu.VMEM((pairs, 2, 16, width // 2), f32),
            pltpu.VMEM((3, pairs, 16, cols), f32),
            sems((nb,)), sems((nb,)), sems((4, nb)), sems((4, nb)), sems((5, nb)), sems((5, nb)),
            sems((2, nsup, 3)), sems((2, nsup, 3)), sems((2,)), sems,
        ],
        compiler_params=pltpu.CompilerParams(
            collective_id=0, has_side_effects=True, vmem_limit_bytes=60 * 1024 * 1024
        ),
    )(pack, weight)[1]


def on_device(l_factor, dinv, weights, tiles):
    zh = lax.axis_index("zh")
    ncol = lax.axis_size("x")
    factor, diag_inv = l_factor[0], dinv[0]
    nsup, rows = factor.shape[1], factor.shape[2]
    width = 2 * rows
    tile_rows = nsup * width // tiles.shape[1]
    expanded = jnp.repeat(tiles.reshape(nsup, nsup, -1), tile_rows, axis=2)
    keep = lax.dynamic_slice_in_dim(expanded, zh * rows, rows, 2).astype(jnp.float32)
    pack = jnp.stack(
        [
            factor[:, row, :, col, :] * keep[col, row][None, :, None] if kind == "L" else diag_inv[:, row]
            for kind, row, col in block_order(nsup)
        ]
    )
    perm = [((l * 2 + k) * 2 + h, ((1 - l) * 2 + h) * 2 + k) for l in range(2) for k in range(2) for h in range(2)]
    weight = lax.ppermute(weights[0], ("zl", "core", "zh"), perm)
    share = window_share(pack, weight, nsup, ncol)

    pairs = [(row, col) for row in range(nsup) for col in range(row + 1)]
    turned = jnp.swapaxes(share, 1, 2)
    low = lax.all_to_all(turned, ("b", "zl", "core"), split_axis=1, concat_axis=2, tiled=True)
    low = low.reshape(*low.shape[:2], 2, 2, 2, 16)
    low = jnp.transpose(low, (0, 1, 4, 2, 3, 5)).reshape(*low.shape[:2], -1)
    off = jnp.stack([share[i] for i, (row, col) in enumerate(pairs) if row > col], axis=0)
    jumps = []
    for a in range(2):
        for b in range(2):
            for l in range(2):
                for k in range(2):
                    for h in range(2):
                        for c in range(ncol):
                            src = ((((a * 2 + b) * 2 + l) * 2 + k) * 2 + h) * ncol + c
                            d = (c % 2, k, b, l, c // 2, h * 2 + a)
                            dst = ((((d[0] * 2 + d[1]) * 2 + d[2]) * 2 + d[3]) * 2 + d[4]) * ncol + d[5]
                            jumps.append((src, dst))
    mirrored = lax.ppermute(off, AXES, jumps)

    spot = {pair: i for i, pair in enumerate(pairs)}
    offs = {pair: i for i, pair in enumerate(p for p in pairs if p[0] > p[1])}
    grid = [
        jnp.stack([low[spot[(row, col)]] if row >= col else mirrored[offs[(col, row)]] for col in range(nsup)], axis=1)
        for row in range(nsup)
    ]
    return jnp.stack(grid)[:, None]


def solution(mesh):
    fine = Mesh(mesh.devices.reshape(2, 2, 2, 2, 2, 4), AXES)
    pole = ("a", "b", "zl", "core")
    return jax.shard_map(
        on_device,
        mesh=fine,
        in_specs=(P(pole, None, None, "zh", None, "x"), P(pole, None, None, "zh", "x"), P(pole, None), P()),
        out_specs=P(None, "zh", pole, None, "x"),
        check_vma=False,
    )
```

```python
import functools

import jax
import jax.numpy as jnp
from jax import lax
from jax.experimental import pallas as pl
from jax.experimental.pallas import tpu as pltpu
from jax.sharding import Mesh
from jax.sharding import PartitionSpec as P

AXES = ("a", "b", "zl", "core", "zh", "x")
MESH = pl.DeviceIdType.MESH


def block_order(nsup):
    lower = [("L", row, col) for col in range(1, nsup - 1) for row in range(col + 1, nsup)]
    diag = [("D", col, col) for col in range(nsup - 1, 0, -1)]
    first = [("L", row, 0) for row in range(1, nsup)]
    return lower + diag + first + [("D", 0, 0)]


def tri(row):
    return row * (row + 1) // 2


def off(nsup, row):
    return tri(nsup) - tri(row + 1)


def split(value):
    high = value.astype(jnp.bfloat16)
    return high, (value - high.astype(jnp.float32)).astype(jnp.bfloat16)


def dot(a, b, dim):
    return lax.dot_general(a, b, (((1,), (dim,)), ((), ())), preferred_element_type=jnp.float32)


def window_kernel(
    nsup, pack, weight, full, out,
    weigh, blk, own_cols, acc_z, acc_g, z_high, z_low, g_high, g_low, real, part1, sum1, part2, share, mirror,
    low_from, low_to,
    z_send, z_recv, x_send, x_recv, c_send, c_recv, r_send, r_recv, m_send, m_recv, l_send, l_recv, w_sems,
    blk_sem, own_sem,
):
    order = block_order(nsup)
    where = {item: i for i, item in enumerate(order)}
    nb = len(order)
    last = nb - 1
    first0 = where[("L", 1, 0)]
    a_, b_, zl, core, zh, x = (lax.axis_index(n) for n in AXES)
    ncol = lax.axis_size("x")
    rows, cols = pack.shape[2], pack.shape[3]
    width = full.shape[2]
    half_w = width // 2
    n = cols // 2
    unit = 2 * n
    right, left, far = lax.rem(x + 1, ncol), lax.rem(x + ncol - 1, ncol), lax.rem(x + 2, ncol)
    to_z = {"zl": 1 - zl, "core": zh, "zh": core}
    to_right, to_left, to_core = {"x": right}, {"x": left}, {"core": 1 - core}

    def other(value, flag):
        return 1 - value if flag else value

    z_peers = [(other(zh, d >> 1), other(zl, d & 1)) for d in (1, 2, 3)]
    y_peers = [(other(a_, d >> 1), other(b_, d & 1)) for d in (1, 2, 3)]
    barrier = pltpu.get_barrier_semaphore()
    peers = [to_z, to_right, to_left, to_core]
    peers += [{"zh": h, "zl": l} for h, l in z_peers] + [{"a": p, "b": q} for p, q in y_peers]
    l_peers = [(other(b_, d >> 2), other(zl, (d >> 1) & 1), other(core, d & 1)) for d in range(1, 8)]
    peers += [{"b": i, "zl": j, "core": k} for i, j, k in l_peers]
    place = 4 * b_ + 2 * zl + core
    goes_to = (lax.rem(x, 2), core, b_, zl, x // 2, zh * 2 + a_)
    comes_from = (lax.rem(x, 2), zl, core, b_, x // 2, zh * 2 + a_)
    stays = (a_ == goes_to[0]) & (b_ == core) & (zl == b_) & (zh == goes_to[4]) & (x == goes_to[5])
    moves = jnp.logical_not(stays)
    peers += [dict(zip(AXES, goes_to)), dict(zip(AXES, comes_from))]
    for peer in peers:
        pl.semaphore_signal(barrier, inc=1, device_id=peer, device_id_type=MESH)

    pl.semaphore_wait(barrier, len(peers))

    both, half0, half1 = pl.ds(0, 2), pl.ds(0, 1), pl.ds(1, 1)

    def tile(b, row, col, parts=both):
        return full.at[
            b,
            parts,
            pl.ds(pl.multiple_of(row * rows, rows), rows),
            pl.ds(pl.multiple_of(col * cols, cols), cols),
        ]

    def remote(src, dst, send, recv, peer):
        return pltpu.make_async_remote_copy(src, dst, send, recv, device_id=peer, device_id_type=MESH)

    def z_copy(b, row):
        return remote(pack.at[b], tile(b, row, x), z_send.at[b], z_recv.at[b], to_z)

    def x_copy(b, kind, col, parts, peer):
        ref = tile(b, core, col, parts)
        return remote(ref, ref, x_send.at[kind, b], x_recv.at[kind, b], peer)

    def c_copy(b, kind, col, parts, row):
        ref = tile(b, row, col, parts)
        return remote(ref, ref, c_send.at[kind, b], c_recv.at[kind, b], to_core)

    c_kinds = ((0, x, both), (1, left, both), (2, right, both), (3, far, half0), (4, far, half1))

    z_order, late = [0, 1], list(range(first0, nb))
    for b in range(2, first0):
        z_order.append(b)
        if late:
            z_order.append(late.pop(0))
    z_order += late
    w_copy = remote(weight, weigh, w_sems.at[0], w_sems.at[1], to_z)
    w_copy.start()
    for b in z_order:
        z_copy(b, zh).start()

    def own_part(b):
        z_copy(b, core).wait_recv()
        c_copy(b, 0, x, both, core).start()

    def own(b):
        if b < first0:
            own_part(b)
        x_copy(b, 0, x, both, to_right).start()
        x_copy(b, 1, x, both, to_left).start()

    def pass_on(b):
        x_copy(b, 0, left, both, to_right).wait_recv()
        x_copy(b, 2, left, half0, to_right).start()
        c_copy(b, 1, left, both, core).start()
        x_copy(b, 1, right, both, to_left).wait_recv()
        x_copy(b, 3, right, half1, to_left).start()
        c_copy(b, 2, right, both, core).start()

    def finish(b):
        x_copy(b, 2, far, half0, to_right).wait_recv()
        c_copy(b, 3, far, half0, core).start()
        x_copy(b, 3, far, half1, to_left).wait_recv()
        c_copy(b, 4, far, half1, core).start()

    ahead = 4

    def service(s):
        if s + ahead < last:
            own(s + ahead)
        if 1 <= s and first0 + s - 1 <= last:
            own_part(first0 + s - 1)
        if s < last:
            pass_on(s)
        if 1 <= s <= last:
            finish(s - 1)

    def arrived(b):
        for kind, col, parts in c_kinds:
            if kind > 0 or b < first0:
                c_copy(b, kind, col, parts, 1 - core).wait_recv()

    def blk_copy(b, slot):
        return pltpu.make_async_copy(full.at[b], blk.at[slot], blk_sem.at[slot])

    def unit_rows(index):
        return pl.ds(pl.multiple_of(index * unit, unit), unit)

    def own_copy(i):
        columns = pl.ds(pl.multiple_of(x * cols, cols), cols)
        return pltpu.make_async_copy(full.at[first0 + i, :, :, columns], own_cols.at[i], own_sem.at[i])

    def set_first(acc, index, i):
        lane = lax.broadcasted_iota(jnp.int32, (n, cols), 1)
        line = lax.broadcasted_iota(jnp.int32, (n, cols), 0)
        pick = jnp.where(lane == line + core * n, 1.0, 0.0).astype(jnp.bfloat16)
        for q in range(2):
            high, low = split(own_cols[i, q])
            acc[0, pl.ds(index * unit + q * n, n), :] = dot(pick, high, 1) + dot(pick, low, 1)
        acc[1, pl.ds(index * unit, unit), :] = jnp.zeros((unit, width), jnp.float32)

    def begin():
        for i in range(nsup):
            c_copy(first0 + i, 0, x, both, 1 - core).wait_recv()
            own_copy(i).start()
        for i in range(nsup):
            own_copy(i).wait()
        for row in range(1, nsup):
            set_first(acc_z, tri(row - 1), row - 1)
        finish_z(1)

    def joined(acc, index):
        p, q = acc[0, unit_rows(index), :], acc[1, unit_rows(index), :]
        return p[:n] - q[n:], p[n:] + q[:n]

    def finish_z(row):
        @pl.loop(0, row)
        def _(k):
            re, im = joined(acc_z, tri(row - 1) + k)
            high, low = split(-jnp.concatenate([re, im], axis=0))
            z_high[unit_rows(tri(row) + k), :] = high
            z_low[unit_rows(tri(row) + k), :] = low

        lane = lax.broadcasted_iota(jnp.int32, (unit, width), 1)
        line = lax.broadcasted_iota(jnp.int32, (unit, width), 0)
        hit = (lane == line + x * cols + core * n) & (line < n)
        z_high[pl.ds((tri(row) + row) * unit, unit), :] = jnp.where(hit, 1.0, 0.0).astype(jnp.bfloat16)
        z_low[pl.ds((tri(row) + row) * unit, unit), :] = jnp.zeros((unit, width), jnp.bfloat16)

    def multiply(acc, acc_at, high, low, at, units, slot, transposed, fresh):
        m, kept = units * unit, (units - fresh) * unit
        here = pl.ds(at * unit, m)

        @pl.loop(0, 2)
        def _(q):
            right_high, right_low = split(blk[slot, q])
            dim = 1 if transposed else 0
            upper = high[here, :]
            total = dot(jnp.concatenate([upper, low[here, :]], axis=0), right_high, dim)
            total = total[:m] + total[m:] + dot(upper, right_low, dim)
            if kept:
                acc[q, pl.ds(acc_at * unit, kept), :] += total[:kept]
            if fresh:
                acc[q, pl.ds(acc_at * unit + kept, fresh * unit), :] = total[kept:]

    def forward(row, mid, slot):
        multiply(acc_z, tri(row - 1), z_high, z_low, tri(mid), mid + 1, slot, True, 1)
        if row == nsup - 1:
            finish_z(mid + 1)

    def backward(row, low_row, slot):
        if low_row == row:
            multiply(acc_g, 0, z_high, z_low, tri(row), row + 1, slot, False, row + 1)
        else:
            multiply(acc_g, 0, g_high, g_low, tri(low_row), row + 1, slot, False, 0)

    def finish_g(row):
        w_re, w_im = weigh[0:1, :], weigh[1:2, :]

        @pl.loop(0, row + 1)
        def _(k):
            re, im = joined(acc_g, k)
            real[off(nsup, row) + k] = (w_re * re - w_im * im).reshape(real.shape[1:])
            if row > 0:
                high, low = split(-jnp.concatenate([re, im], axis=0))
                g_high[unit_rows(tri(row) + k), :] = high
                g_low[unit_rows(tri(row) + k), :] = low

        for copy in first_stage(row):
            copy.start()

    def first_stage(row):
        span = pl.ds(off(nsup, row), row + 1)
        copies = []
        for d, (h, l) in enumerate(z_peers):
            lanes = pl.ds(pl.multiple_of(h * half_w, half_w), half_w)
            copies.append(
                remote(
                    real.at[span, :, l, :, lanes], part1.at[d, span], r_send.at[0, row, d], r_recv.at[0, row, d],
                    {"zh": h, "zl": l},
                )
            )
        return copies

    def second_stage(row):
        span = pl.ds(off(nsup, row), row + 1)
        copies = []
        for d, (p, q) in enumerate(y_peers):
            lanes = pl.ds(pl.multiple_of(p * cols, cols), cols)
            copies.append(
                remote(
                    sum1.at[span, q, :, lanes], part2.at[d, span], r_send.at[1, row, d], r_recv.at[1, row, d],
                    {"a": p, "b": q},
                )
            )
        return copies

    def reduce_first(row):
        for copy in first_stage(row):
            copy.wait_recv()
        span = pl.ds(off(nsup, row), row + 1)
        lanes = pl.ds(pl.multiple_of(zh * half_w, half_w), half_w)
        sum1[span] = real[span, :, zl, :, lanes] + part1[0, span] + part1[1, span] + part1[2, span]
        for copy in second_stage(row):
            copy.start()

    def reduce_second(row):
        for copy in second_stage(row):
            copy.wait_recv()
        span = pl.ds(off(nsup, row), row + 1)
        lanes = pl.ds(pl.multiple_of(a_ * cols, cols), cols)
        share[span] = sum1[span, b_, :, lanes] + part2[0, span] + part2[1, span] + part2[2, span]
        if row > 0:

            @pl.when(moves)
            def _():
                mirror_copy(row).start()

        if row == 2:
            start_low(0)
            start_low(1)
        if row == 0:
            start_low(2)

    def mirror_copy(row):
        span = pl.ds(off(nsup, row), row)
        return remote(
            share.at[span], mirror.at[span], m_send.at[row], m_recv.at[row], dict(zip(AXES, goes_to))
        )

    def low_copies(g):
        copies = []
        for d, (i, j, k) in enumerate(l_peers):
            lines = pl.ds(pl.multiple_of((4 * i + 2 * j + k) * 16, 16), 16)
            copies.append(
                remote(
                    low_from.at[g, lines], low_to.at[g, place], l_send.at[g, d], l_recv.at[g, d],
                    {"b": i, "zl": j, "core": k},
                )
            )
        return copies

    def start_low(g):
        low_from[g] = jnp.transpose(share[pl.ds(8 * g, 8)].reshape(cols, cols))
        low_to[g, place] = low_from[g, pl.ds(pl.multiple_of(place * 16, 16), 16), :]
        for copy in low_copies(g):
            copy.start()

    def finish_low(g):
        for copy in low_copies(g):
            copy.wait_recv()
        places = [4 * j + 2 * k + i for i in range(2) for j in range(2) for k in range(2)]
        for row in range(nsup):
            for col in range(row + 1):
                p = off(nsup, row) + col - 8 * g
                if 0 <= p < 8:
                    pieces = [low_to[g, s, :, p * 16 : p * 16 + 16] for s in places]
                    out[row, col] = jnp.concatenate(pieces, axis=1)

    def finish_mirror():
        @pl.when(moves)
        def _():
            for row in range(1, nsup):
                mirror_copy(row).wait_recv()

        @pl.when(stays)
        def _():
            mirror[...] = share[pl.ds(0, tri(nsup))]

        for row in range(1, nsup):
            for col in range(row):
                out[col, row] = mirror[off(nsup, row) + col]


    items = []
    for b in range(nsup * (nsup - 1) // 2 - (nsup - 1)):
        kind, row, mid = order[b]
        items.append((functools.partial(forward, row, mid), b, b, mid))
    for row in range(nsup - 1, 0, -1):
        items.append((functools.partial(backward, row, row), where[("D", row, row)], where[("D", row, row)], row + 1))
        for low_row in range(row + 1, nsup):
            items.append(
                (functools.partial(backward, row, low_row), where[("L", low_row, row)], where[("D", row, row)], row + 1)
            )
    for low_row in range(1, nsup):
        b = where[("L", low_row, 0)]
        items.append((functools.partial(backward, 0, low_row), b, b, 1))

    for i in range(24 - tri(nsup)):
        share[tri(nsup) + i] = jnp.zeros(share.shape[1:], jnp.float32)
    for b in range(ahead):
        own(b)
    state = {"done": -1, "loaded": -1}
    seen = set()

    def fetch(i):
        if i <= state["loaded"] or i >= len(items) or items[i][2] + 1 > state["done"]:
            return
        b = items[i][1]
        if b not in seen:
            seen.add(b)
            arrived(b)
        blk_copy(b, i % 2).start()
        state["loaded"] = i

    todo, started, summed = 0, [], []
    ready_at = first0 - where[("L", 1, 0)] + nsup + 1
    finals = {}
    for i, (fn, b, avail, units) in enumerate(items):
        if fn.func is backward and fn.args[1] == nsup - 1:
            finals[i] = fn.args[0]
    for s in range(last + 1):
        service(s)
        state["done"] = s
        if s == ready_at:
            begin()
        if s < ready_at:
            continue
        for row in summed:
            reduce_second(row)
        summed = list(started)
        for row in started:
            reduce_first(row)
        started = []
        budget = 6 if s < last else 10**6
        while todo < len(items) and items[todo][2] + 1 <= s and budget > 0:
            fetch(todo)
            fetch(todo + 1)
            blk_copy(items[todo][1], todo % 2).wait()
            if todo == len(items) - nsup + 1:
                set_first(acc_g, 0, nsup - 1)
            items[todo][0](todo % 2)
            budget -= items[todo][3]
            if todo in finals:
                if finals[todo] == nsup - 1:
                    w_copy.wait_recv()
                finish_g(finals[todo])
                started.append(finals[todo])
            todo += 1
    for row in summed:
        reduce_second(row)
    for row in started:
        reduce_first(row)
    for row in started:
        reduce_second(row)
    for g in range(3):
        finish_low(g)
    finish_mirror()

    w_copy.wait_send()
    for g in range(3):
        for copy in low_copies(g):
            copy.wait_send()

    @pl.when(moves)
    def _():
        for row in range(1, nsup):
            mirror_copy(row).wait_send()

    for b in range(nb):
        z_copy(b, zh).wait_send()
        c_copy(b, 0, x, both, core).wait_send()
        if b < last:
            x_copy(b, 0, x, both, to_right).wait_send()
            x_copy(b, 1, x, both, to_left).wait_send()
            x_copy(b, 2, left, half0, to_right).wait_send()
            x_copy(b, 3, right, half1, to_left).wait_send()
            for kind, col, parts in c_kinds[1:]:
                c_copy(b, kind, col, parts, core).wait_send()
    for row in range(nsup):
        for copy in first_stage(row) + second_stage(row):
            copy.wait_send()


def window_share(pack, weight, nsup, ncol):
    nb, parts, rows, cols = pack.shape
    width, unit, pairs = 2 * rows, cols, tri(nsup)
    sems = pltpu.SemaphoreType.DMA
    f32, bf16 = jnp.float32, jnp.bfloat16
    return pl.pallas_call(
        functools.partial(window_kernel, nsup),
        out_shape=(
            jax.ShapeDtypeStruct((nb, parts, width, width), f32),
            jax.ShapeDtypeStruct((nsup, nsup, 16, cols), f32),
        ),
        in_specs=[pl.BlockSpec(memory_space=pl.ANY), pl.BlockSpec(memory_space=pltpu.VMEM)],
        out_specs=(pl.BlockSpec(memory_space=pl.ANY), pl.BlockSpec(memory_space=pltpu.VMEM)),
        scratch_shapes=[
            pltpu.VMEM(weight.shape, f32),
            pltpu.VMEM((2, parts, width, width), f32),
            pltpu.VMEM((nsup, parts, width, cols), f32),
            pltpu.VMEM((2, tri(nsup - 1) * unit, width), f32),
            pltpu.VMEM((2, nsup * unit, width), f32),
            pltpu.VMEM((pairs * unit, width), bf16),
            pltpu.VMEM((pairs * unit, width), bf16),
            pltpu.VMEM((pairs * unit, width), bf16),
            pltpu.VMEM((pairs * unit, width), bf16),
            pltpu.VMEM((pairs, 2, 2, 16, width), f32),
            pltpu.VMEM((3, pairs, 2, 16, width // 2), f32),
            pltpu.VMEM((pairs, 2, 16, width // 2), f32),
            pltpu.VMEM((3, pairs, 16, cols), f32),
            pltpu.VMEM((24, 16, cols), f32),
            pltpu.VMEM((pairs, 16, cols), f32),
            pltpu.VMEM((3, cols, cols), f32),
            pltpu.VMEM((3, 8, 16, cols), f32),
            sems((nb,)), sems((nb,)), sems((4, nb)), sems((4, nb)), sems((5, nb)), sems((5, nb)),
            sems((2, nsup, 3)), sems((2, nsup, 3)), sems((nsup,)), sems((nsup,)), sems((3, 7)), sems((3, 7)), sems((2,)),
            sems((2,)), sems((nsup,)),
        ],
        compiler_params=pltpu.CompilerParams(
            collective_id=0, has_side_effects=True, vmem_limit_bytes=60 * 1024 * 1024
        ),
    )(pack, weight)[1]


def on_device(l_factor, dinv, weights, tiles):
    zh = lax.axis_index("zh")
    ncol = lax.axis_size("x")
    factor, diag_inv = l_factor[0], dinv[0]
    nsup, rows = factor.shape[1], factor.shape[2]
    width = 2 * rows
    tile_rows = nsup * width // tiles.shape[1]
    expanded = jnp.repeat(tiles.reshape(nsup, nsup, -1), tile_rows, axis=2)
    keep = lax.dynamic_slice_in_dim(expanded, zh * rows, rows, 2).astype(jnp.float32)
    pack = jnp.stack(
        [
            factor[:, row, :, col, :] * keep[col, row][None, :, None] if kind == "L" else diag_inv[:, row]
            for kind, row, col in block_order(nsup)
        ]
    )
    weight = jnp.broadcast_to(jnp.pad(weights[0], (0, 6))[:, None], (8, width))
    blocks = window_share(pack, weight, nsup, ncol)
    return jnp.transpose(blocks, (0, 2, 1, 3))[:, None]


def solution(mesh):
    fine = Mesh(mesh.devices.reshape(2, 2, 2, 2, 2, 4), AXES)
    pole = ("a", "b", "zl", "core")
    return jax.shard_map(
        on_device,
        mesh=fine,
        in_specs=(P(pole, None, None, "zh", None, "x"), P(pole, None, None, "zh", "x"), P(pole, None), P()),
        out_specs=P(None, "zh", pole, None, "x"),
        check_vma=False,
    )
```

```python
import functools

import jax
import jax.numpy as jnp
from jax import lax
from jax.experimental import pallas as pl
from jax.experimental.pallas import tpu as pltpu
from jax.sharding import Mesh
from jax.sharding import PartitionSpec as P

AXES = ("a", "b", "zl", "core", "zh", "x")
MESH = pl.DeviceIdType.MESH


def block_order(nsup):
    lower = [("L", row, col) for col in range(1, nsup - 1) for row in range(col + 1, nsup)]
    diag = [("D", col, col) for col in range(nsup - 1, 0, -1)]
    first = [("L", row, 0) for row in range(1, nsup)]
    return lower + diag + first + [("D", 0, 0)]


def tri(row):
    return row * (row + 1) // 2


def off(nsup, row):
    return tri(nsup) - tri(row + 1)


def split(value):
    high = value.astype(jnp.bfloat16)
    return high, (value - high.astype(jnp.float32)).astype(jnp.bfloat16)


def dot(a, b, dim):
    return lax.dot_general(a, b, (((1,), (dim,)), ((), ())), preferred_element_type=jnp.float32)


def window_kernel(
    nsup, factor, dinv, tiles, weight, full, out,
    pack, weigh, blk, own_cols, acc_z, acc_g, z_high, z_low, g_high, g_low, real, part1, sum1, part2, share, mirror,
    low_from, low_to,
    z_send, z_recv, x_send, x_recv, c_send, c_recv, r_send, r_recv, m_send, m_recv, l_send, l_recv, w_sems,
    blk_sem, own_sem, pack_sem,
):
    order = block_order(nsup)
    where = {item: i for i, item in enumerate(order)}
    nb = len(order)
    last = nb - 1
    first0 = where[("L", 1, 0)]
    a_, b_, zl, core, zh, x = (lax.axis_index(n) for n in AXES)
    ncol = lax.axis_size("x")
    rows, cols = pack.shape[2], pack.shape[3]
    width = full.shape[2]
    half_w = width // 2
    n = cols // 2
    unit = 2 * n
    right, left, far = lax.rem(x + 1, ncol), lax.rem(x + ncol - 1, ncol), lax.rem(x + 2, ncol)
    to_z = {"zl": 1 - zl, "core": zh, "zh": core}
    to_right, to_left, to_core = {"x": right}, {"x": left}, {"core": 1 - core}

    def other(value, flag):
        return 1 - value if flag else value

    z_peers = [(other(zh, d >> 1), other(zl, d & 1)) for d in (1, 2, 3)]
    y_peers = [(other(a_, d >> 1), other(b_, d & 1)) for d in (1, 2, 3)]
    barrier = pltpu.get_barrier_semaphore()
    peers = [to_z, to_right, to_left, to_core]
    peers += [{"zh": h, "zl": l} for h, l in z_peers] + [{"a": p, "b": q} for p, q in y_peers]
    l_peers = [(other(b_, d >> 2), other(zl, (d >> 1) & 1), other(core, d & 1)) for d in range(1, 8)]
    peers += [{"b": i, "zl": j, "core": k} for i, j, k in l_peers]
    place = 4 * b_ + 2 * zl + core
    goes_to = (lax.rem(x, 2), core, b_, zl, x // 2, zh * 2 + a_)
    comes_from = (lax.rem(x, 2), zl, core, b_, x // 2, zh * 2 + a_)
    stays = (a_ == goes_to[0]) & (b_ == core) & (zl == b_) & (zh == goes_to[4]) & (x == goes_to[5])
    moves = jnp.logical_not(stays)
    peers += [dict(zip(AXES, goes_to)), dict(zip(AXES, comes_from))]
    for peer in peers:
        pl.semaphore_signal(barrier, inc=1, device_id=peer, device_id_type=MESH)

    pl.semaphore_wait(barrier, len(peers))

    both, half0, half1 = pl.ds(0, 2), pl.ds(0, 1), pl.ds(1, 1)

    def tile(b, row, col, parts=both):
        return full.at[
            b,
            parts,
            pl.ds(pl.multiple_of(row * rows, rows), rows),
            pl.ds(pl.multiple_of(col * cols, cols), cols),
        ]

    def remote(src, dst, send, recv, peer):
        return pltpu.make_async_remote_copy(src, dst, send, recv, device_id=peer, device_id_type=MESH)

    def z_copy(b, row):
        return remote(pack.at[b], tile(b, row, x), z_send.at[b], z_recv.at[b], to_z)

    def x_copy(b, kind, col, parts, peer):
        ref = tile(b, core, col, parts)
        return remote(ref, ref, x_send.at[kind, b], x_recv.at[kind, b], peer)

    def c_copy(b, kind, col, parts, row):
        ref = tile(b, row, col, parts)
        return remote(ref, ref, c_send.at[kind, b], c_recv.at[kind, b], to_core)

    c_kinds = ((0, x, both), (1, left, both), (2, right, both), (3, far, half0), (4, far, half1))

    z_order, late = [0, 1], list(range(first0, nb))
    for b in range(2, first0):
        z_order.append(b)
        if late:
            z_order.append(late.pop(0))
    z_order += late
    w_copy = remote(weight, weigh, w_sems.at[0], w_sems.at[1], to_z)
    w_copy.start()

    def pack_copy(b):
        kind, row, col = order[b]
        source = factor.at[0, :, row, :, col, :] if kind == "L" else dinv.at[0, :, row]
        return pltpu.make_async_copy(source, pack.at[b], pack_sem.at[b])

    def masked(b):
        kind, row, col = order[b]
        if kind == "L":
            per_block = tiles.shape[1] // nsup
            here = per_block // 2
            size = rows // here

            @pl.loop(0, 2 * here)
            def _(i):
                q, t = i // here, lax.rem(i, here)
                keep = tiles[col, row * per_block + zh * here + t].astype(jnp.float32)
                lines = pl.ds(pl.multiple_of(t * size, size), size)
                pack[b, q, lines, :] = pack[b, q, lines, :] * keep

    for b in z_order:
        pack_copy(b).start()
    for b in z_order:
        pack_copy(b).wait()
        masked(b)
        z_copy(b, zh).start()

    def own_part(b):
        z_copy(b, core).wait_recv()
        c_copy(b, 0, x, both, core).start()

    def own(b):
        if b < first0:
            own_part(b)
        x_copy(b, 0, x, both, to_right).start()
        x_copy(b, 1, x, both, to_left).start()

    def pass_on(b):
        x_copy(b, 0, left, both, to_right).wait_recv()
        x_copy(b, 2, left, half0, to_right).start()
        c_copy(b, 1, left, both, core).start()
        x_copy(b, 1, right, both, to_left).wait_recv()
        x_copy(b, 3, right, half1, to_left).start()
        c_copy(b, 2, right, both, core).start()

    def finish(b):
        x_copy(b, 2, far, half0, to_right).wait_recv()
        c_copy(b, 3, far, half0, core).start()
        x_copy(b, 3, far, half1, to_left).wait_recv()
        c_copy(b, 4, far, half1, core).start()

    ahead, delay, pace = 2, 3, 8

    def service(s):
        if s + ahead < last:
            own(s + ahead)
        if 1 <= s and first0 + s - 1 <= last:
            own_part(first0 + s - 1)
        if s < last:
            pass_on(s)
        if ahead <= s < last + ahead:
            finish(s - ahead)

    def arrived(b):
        for kind, col, parts in c_kinds:
            if kind > 0 or b < first0:
                c_copy(b, kind, col, parts, 1 - core).wait_recv()

    def blk_copy(b, slot):
        return pltpu.make_async_copy(full.at[b], blk.at[slot], blk_sem.at[slot])

    def unit_rows(index):
        return pl.ds(pl.multiple_of(index * unit, unit), unit)

    def own_copy(i):
        columns = pl.ds(pl.multiple_of(x * cols, cols), cols)
        return pltpu.make_async_copy(full.at[first0 + i, :, :, columns], own_cols.at[i], own_sem.at[i])

    def set_first(acc, index, i):
        lane = lax.broadcasted_iota(jnp.int32, (n, cols), 1)
        line = lax.broadcasted_iota(jnp.int32, (n, cols), 0)
        pick = jnp.where(lane == line + core * n, 1.0, 0.0).astype(jnp.bfloat16)
        for q in range(2):
            high, low = split(own_cols[i, q])
            acc[0, pl.ds(index * unit + q * n, n), :] = dot(pick, high, 1) + dot(pick, low, 1)
        acc[1, pl.ds(index * unit, unit), :] = jnp.zeros((unit, width), jnp.float32)

    def begin():
        for i in range(nsup):
            c_copy(first0 + i, 0, x, both, 1 - core).wait_recv()
            own_copy(i).start()
        for i in range(nsup):
            own_copy(i).wait()
        for row in range(1, nsup):
            set_first(acc_z, tri(row - 1), row - 1)
        finish_z(1)

    def joined(acc, index):
        p, q = acc[0, unit_rows(index), :], acc[1, unit_rows(index), :]
        return p[:n] - q[n:], p[n:] + q[:n]

    def finish_z(row):
        @pl.loop(0, row)
        def _(k):
            re, im = joined(acc_z, tri(row - 1) + k)
            high, low = split(-jnp.concatenate([re, im], axis=0))
            z_high[unit_rows(tri(row) + k), :] = high
            z_low[unit_rows(tri(row) + k), :] = low

        lane = lax.broadcasted_iota(jnp.int32, (unit, width), 1)
        line = lax.broadcasted_iota(jnp.int32, (unit, width), 0)
        hit = (lane == line + x * cols + core * n) & (line < n)
        z_high[pl.ds((tri(row) + row) * unit, unit), :] = jnp.where(hit, 1.0, 0.0).astype(jnp.bfloat16)
        z_low[pl.ds((tri(row) + row) * unit, unit), :] = jnp.zeros((unit, width), jnp.bfloat16)

    def multiply(acc, acc_at, high, low, at, units, slot, transposed, fresh):
        m, kept = units * unit, (units - fresh) * unit
        here = pl.ds(at * unit, m)

        @pl.loop(0, 2)
        def _(q):
            right_high, right_low = split(blk[slot, q])
            dim = 1 if transposed else 0
            upper = high[here, :]
            total = dot(jnp.concatenate([upper, low[here, :]], axis=0), right_high, dim)
            total = total[:m] + total[m:] + dot(upper, right_low, dim)
            if kept:
                acc[q, pl.ds(acc_at * unit, kept), :] += total[:kept]
            if fresh:
                acc[q, pl.ds(acc_at * unit + kept, fresh * unit), :] = total[kept:]

    def forward(row, mid, slot):
        multiply(acc_z, tri(row - 1), z_high, z_low, tri(mid), mid + 1, slot, True, 1)
        if row == nsup - 1:
            finish_z(mid + 1)

    def backward(row, low_row, slot):
        if low_row == row:
            multiply(acc_g, 0, z_high, z_low, tri(row), row + 1, slot, False, row + 1)
        else:
            multiply(acc_g, 0, g_high, g_low, tri(low_row), row + 1, slot, False, 0)

    def finish_g(row):
        w_re, w_im = weigh[0:1, :], weigh[1:2, :]

        @pl.loop(0, row + 1)
        def _(k):
            re, im = joined(acc_g, k)
            real[off(nsup, row) + k] = (w_re * re - w_im * im).reshape(real.shape[1:])
            if row > 0:
                high, low = split(-jnp.concatenate([re, im], axis=0))
                g_high[unit_rows(tri(row) + k), :] = high
                g_low[unit_rows(tri(row) + k), :] = low

        for copy in first_stage(row):
            copy.start()

    def first_stage(row):
        span = pl.ds(off(nsup, row), row + 1)
        copies = []
        for d, (h, l) in enumerate(z_peers):
            lanes = pl.ds(pl.multiple_of(h * half_w, half_w), half_w)
            copies.append(
                remote(
                    real.at[span, :, l, :, lanes], part1.at[d, span], r_send.at[0, row, d], r_recv.at[0, row, d],
                    {"zh": h, "zl": l},
                )
            )
        return copies

    def second_stage(row):
        span = pl.ds(off(nsup, row), row + 1)
        copies = []
        for d, (p, q) in enumerate(y_peers):
            lanes = pl.ds(pl.multiple_of(p * cols, cols), cols)
            copies.append(
                remote(
                    sum1.at[span, q, :, lanes], part2.at[d, span], r_send.at[1, row, d], r_recv.at[1, row, d],
                    {"a": p, "b": q},
                )
            )
        return copies

    def reduce_first(row):
        for copy in first_stage(row):
            copy.wait_recv()
        span = pl.ds(off(nsup, row), row + 1)
        lanes = pl.ds(pl.multiple_of(zh * half_w, half_w), half_w)
        sum1[span] = real[span, :, zl, :, lanes] + part1[0, span] + part1[1, span] + part1[2, span]
        for copy in second_stage(row):
            copy.start()

    def reduce_second(row):
        for copy in second_stage(row):
            copy.wait_recv()
        span = pl.ds(off(nsup, row), row + 1)
        lanes = pl.ds(pl.multiple_of(a_ * cols, cols), cols)
        share[span] = sum1[span, b_, :, lanes] + part2[0, span] + part2[1, span] + part2[2, span]
        if row > 0:

            @pl.when(moves)
            def _():
                mirror_copy(row).start()

        if row == 2:
            start_low(0)
            start_low(1)
        if row == 0:
            start_low(2)

    def mirror_copy(row):
        span = pl.ds(off(nsup, row), row)
        return remote(
            share.at[span], mirror.at[span], m_send.at[row], m_recv.at[row], dict(zip(AXES, goes_to))
        )

    def low_copies(g):
        copies = []
        for d, (i, j, k) in enumerate(l_peers):
            lines = pl.ds(pl.multiple_of((4 * i + 2 * j + k) * 16, 16), 16)
            copies.append(
                remote(
                    low_from.at[g, lines], low_to.at[g, place], l_send.at[g, d], l_recv.at[g, d],
                    {"b": i, "zl": j, "core": k},
                )
            )
        return copies

    def start_low(g):
        low_from[g] = jnp.transpose(share[pl.ds(8 * g, 8)].reshape(cols, cols))
        low_to[g, place] = low_from[g, pl.ds(pl.multiple_of(place * 16, 16), 16), :]
        for copy in low_copies(g):
            copy.start()

    def finish_low(g):
        for copy in low_copies(g):
            copy.wait_recv()
        places = [4 * j + 2 * k + i for i in range(2) for j in range(2) for k in range(2)]
        for row in range(nsup):
            for col in range(row + 1):
                p = off(nsup, row) + col - 8 * g
                if 0 <= p < 8:
                    pieces = [low_to[g, s, :, p * 16 : p * 16 + 16] for s in places]
                    out[row, col] = jnp.concatenate(pieces, axis=1)

    def finish_mirror():
        @pl.when(moves)
        def _():
            for row in range(1, nsup):
                mirror_copy(row).wait_recv()

        @pl.when(stays)
        def _():
            mirror[...] = share[pl.ds(0, tri(nsup))]

        for row in range(1, nsup):
            for col in range(row):
                out[col, row] = mirror[off(nsup, row) + col]


    items = []
    for b in range(nsup * (nsup - 1) // 2 - (nsup - 1)):
        kind, row, mid = order[b]
        items.append((functools.partial(forward, row, mid), b, b, mid))
    for row in range(nsup - 1, 0, -1):
        items.append((functools.partial(backward, row, row), where[("D", row, row)], where[("D", row, row)], row + 1))
        for low_row in range(row + 1, nsup):
            items.append(
                (functools.partial(backward, row, low_row), where[("L", low_row, row)], where[("D", row, row)], row + 1)
            )
    for low_row in range(1, nsup):
        b = where[("L", low_row, 0)]
        items.append((functools.partial(backward, 0, low_row), b, b, 1))

    for i in range(24 - tri(nsup)):
        share[tri(nsup) + i] = jnp.zeros(share.shape[1:], jnp.float32)
    for b in range(ahead):
        own(b)
    state = {"done": -1, "loaded": -1}
    seen = set()

    def fetch(i):
        if i <= state["loaded"] or i >= len(items) or items[i][2] + ahead > state["done"]:
            return
        b = items[i][1]
        if b not in seen:
            seen.add(b)
            arrived(b)
        blk_copy(b, i % 2).start()
        state["loaded"] = i

    todo, started, summed = 0, [], []
    ready_at = first0 - where[("L", 1, 0)] + nsup + 1
    finals = {}
    for i, (fn, b, avail, units) in enumerate(items):
        if fn.func is backward and fn.args[1] == nsup - 1:
            finals[i] = fn.args[0]
    for s in range(last + ahead):
        service(s)
        state["done"] = s
        if s == ready_at:
            begin()
        if s < ready_at:
            continue
        for row, since in list(summed):
            if s >= since + delay:
                reduce_second(row)
                summed.remove((row, since))
        for row, since in list(started):
            if s >= since + delay:
                reduce_first(row)
                started.remove((row, since))
                summed.append((row, s))
        budget = pace if s < last + ahead - 1 else 10**6
        while todo < len(items) and items[todo][2] + ahead <= s and budget > 0:
            fetch(todo)
            fetch(todo + 1)
            blk_copy(items[todo][1], todo % 2).wait()
            if todo == len(items) - nsup + 1:
                set_first(acc_g, 0, nsup - 1)
            items[todo][0](todo % 2)
            budget -= items[todo][3]
            if todo in finals:
                if finals[todo] == nsup - 1:
                    w_copy.wait_recv()
                finish_g(finals[todo])
                started.append((finals[todo], s))
            todo += 1
    for row, since in started:
        reduce_first(row)
    for row, since in summed + started:
        reduce_second(row)
    for g in range(3):
        finish_low(g)
    finish_mirror()

    w_copy.wait_send()
    for g in range(3):
        for copy in low_copies(g):
            copy.wait_send()

    @pl.when(moves)
    def _():
        for row in range(1, nsup):
            mirror_copy(row).wait_send()

    for b in range(nb):
        z_copy(b, zh).wait_send()
        c_copy(b, 0, x, both, core).wait_send()
        if b < last:
            x_copy(b, 0, x, both, to_right).wait_send()
            x_copy(b, 1, x, both, to_left).wait_send()
            x_copy(b, 2, left, half0, to_right).wait_send()
            x_copy(b, 3, right, half1, to_left).wait_send()
            for kind, col, parts in c_kinds[1:]:
                c_copy(b, kind, col, parts, core).wait_send()
    for row in range(nsup):
        for copy in first_stage(row) + second_stage(row):
            copy.wait_send()


def window_share(factor, dinv, tiles, weight, ncol):
    _, parts, nsup, rows, _, cols = factor.shape
    nb = tri(nsup)
    width, unit, pairs = 2 * rows, cols, tri(nsup)
    sems = pltpu.SemaphoreType.DMA
    f32, bf16 = jnp.float32, jnp.bfloat16
    return pl.pallas_call(
        functools.partial(window_kernel, nsup),
        out_shape=(
            jax.ShapeDtypeStruct((nb, parts, width, width), f32),
            jax.ShapeDtypeStruct((nsup, nsup, 16, cols), f32),
        ),
        in_specs=[
            pl.BlockSpec(memory_space=pl.ANY),
            pl.BlockSpec(memory_space=pl.ANY),
            pl.BlockSpec(memory_space=pltpu.SMEM),
            pl.BlockSpec(memory_space=pltpu.VMEM),
        ],
        out_specs=(pl.BlockSpec(memory_space=pl.ANY), pl.BlockSpec(memory_space=pltpu.VMEM)),
        scratch_shapes=[
            pltpu.VMEM((nb, parts, rows, cols), f32),
            pltpu.VMEM(weight.shape, f32),
            pltpu.VMEM((2, parts, width, width), f32),
            pltpu.VMEM((nsup, parts, width, cols), f32),
            pltpu.VMEM((2, tri(nsup - 1) * unit, width), f32),
            pltpu.VMEM((2, nsup * unit, width), f32),
            pltpu.VMEM((pairs * unit, width), bf16),
            pltpu.VMEM((pairs * unit, width), bf16),
            pltpu.VMEM((pairs * unit, width), bf16),
            pltpu.VMEM((pairs * unit, width), bf16),
            pltpu.VMEM((pairs, 2, 2, 16, width), f32),
            pltpu.VMEM((3, pairs, 2, 16, width // 2), f32),
            pltpu.VMEM((pairs, 2, 16, width // 2), f32),
            pltpu.VMEM((3, pairs, 16, cols), f32),
            pltpu.VMEM((24, 16, cols), f32),
            pltpu.VMEM((pairs, 16, cols), f32),
            pltpu.VMEM((3, cols, cols), f32),
            pltpu.VMEM((3, 8, 16, cols), f32),
            sems((nb,)), sems((nb,)), sems((4, nb)), sems((4, nb)), sems((5, nb)), sems((5, nb)),
            sems((2, nsup, 3)), sems((2, nsup, 3)), sems((nsup,)), sems((nsup,)), sems((3, 7)), sems((3, 7)), sems((2,)),
            sems((2,)), sems((nsup,)), sems((nb,)),
        ],
        compiler_params=pltpu.CompilerParams(
            collective_id=0, has_side_effects=True, vmem_limit_bytes=60 * 1024 * 1024
        ),
    )(factor, dinv, tiles, weight)[1]


def on_device(l_factor, dinv, weights, tiles):
    width = 2 * l_factor.shape[3]
    weight = jnp.broadcast_to(jnp.pad(weights[0], (0, 6))[:, None], (8, width))
    blocks = window_share(l_factor, dinv, tiles, weight, lax.axis_size("x"))
    return jnp.transpose(blocks, (0, 2, 1, 3))[:, None]


def solution(mesh):
    fine = Mesh(mesh.devices.reshape(2, 2, 2, 2, 2, 4), AXES)
    pole = ("a", "b", "zl", "core")
    return jax.shard_map(
        on_device,
        mesh=fine,
        in_specs=(P(pole, None, None, "zh", None, "x"), P(pole, None, None, "zh", "x"), P(pole, None), P()),
        out_specs=P(None, "zh", pole, None, "x"),
        check_vma=False,
    )
```

```python
import functools

import jax
import jax.numpy as jnp
from jax import lax
from jax.experimental import pallas as pl
from jax.experimental.pallas import tpu as pltpu
from jax.sharding import Mesh
from jax.sharding import PartitionSpec as P

AXES = ("a", "b", "zl", "core", "zh", "x")
MESH = pl.DeviceIdType.MESH


def block_order(nsup):
    lower = [("L", row, col) for col in range(1, nsup - 1) for row in range(col + 1, nsup)]
    diag = [("D", col, col) for col in range(nsup - 1, 0, -1)]
    first = [("L", row, 0) for row in range(1, nsup)]
    return lower + diag + first + [("D", 0, 0)]


def tri(row):
    return row * (row + 1) // 2


def off(nsup, row):
    return tri(nsup) - tri(row + 1)


def split(value):
    high = value.astype(jnp.bfloat16)
    return high, (value - high.astype(jnp.float32)).astype(jnp.bfloat16)


def dot(a, b, dim):
    return lax.dot_general(a, b, (((1,), (dim,)), ((), ())), preferred_element_type=jnp.float32)


def window_kernel(
    nsup, factor, dinv, tiles, weight, full, out,
    pack, weigh, blk, own_cols, acc_z, acc_g, z_high, z_low, g_high, g_low, real, part1, sum1, part2, share, mirror,
    low_from, low_to,
    z_send, z_recv, x_send, x_recv, c_send, c_recv, r_send, r_recv, m_send, m_recv, l_send, l_recv, w_sems,
    dx_send, dx_recv, dc_send, dc_recv, blk_sem, own_sem, pack_sem,
):
    order = block_order(nsup)
    where = {item: i for i, item in enumerate(order)}
    nb = len(order)
    last = nb - 1
    first0 = where[("L", 1, 0)]
    a_, b_, zl, core, zh, x = (lax.axis_index(n) for n in AXES)
    ncol = lax.axis_size("x")
    rows, cols = pack.shape[2], pack.shape[3]
    width = full.shape[2]
    half_w = width // 2
    n = cols // 2
    unit = 2 * n
    right, left, far = lax.rem(x + 1, ncol), lax.rem(x + ncol - 1, ncol), lax.rem(x + 2, ncol)
    to_z = {"zl": 1 - zl, "core": zh, "zh": core}
    to_right, to_left, to_core = {"x": right}, {"x": left}, {"core": 1 - core}

    def other(value, flag):
        return 1 - value if flag else value

    z_peers = [(other(zh, d >> 1), other(zl, d & 1)) for d in (1, 2, 3)]
    y_peers = [(other(a_, d >> 1), other(b_, d & 1)) for d in (1, 2, 3)]
    barrier = pltpu.get_barrier_semaphore()
    peers = [to_z, to_right, to_left, to_core]
    peers += [{"zh": h, "zl": l} for h, l in z_peers] + [{"a": p, "b": q} for p, q in y_peers]
    l_peers = [(other(b_, d >> 2), other(zl, (d >> 1) & 1), other(core, d & 1)) for d in range(1, 8)]
    peers += [{"b": i, "zl": j, "core": k} for i, j, k in l_peers]
    place = 4 * b_ + 2 * zl + core
    goes_to = (lax.rem(x, 2), core, b_, zl, x // 2, zh * 2 + a_)
    comes_from = (lax.rem(x, 2), zl, core, b_, x // 2, zh * 2 + a_)
    stays = (a_ == goes_to[0]) & (b_ == core) & (zl == b_) & (zh == goes_to[4]) & (x == goes_to[5])
    moves = jnp.logical_not(stays)
    peers += [dict(zip(AXES, goes_to)), dict(zip(AXES, comes_from))]
    for peer in peers:
        pl.semaphore_signal(barrier, inc=1, device_id=peer, device_id_type=MESH)

    pl.semaphore_wait(barrier, len(peers))

    both, half0, half1 = pl.ds(0, 2), pl.ds(0, 1), pl.ds(1, 1)

    def tile(b, row, col, parts=both):
        return full.at[
            b,
            parts,
            pl.ds(pl.multiple_of(row * rows, rows), rows),
            pl.ds(pl.multiple_of(col * cols, cols), cols),
        ]

    def remote(src, dst, send, recv, peer):
        return pltpu.make_async_remote_copy(src, dst, send, recv, device_id=peer, device_id_type=MESH)

    def z_copy(b, row):
        return remote(pack.at[b], tile(b, row, x), z_send.at[b], z_recv.at[b], to_z)

    def x_copy(b, kind, col, parts, peer):
        ref = tile(b, core, col, parts)
        return remote(ref, ref, x_send.at[kind, b], x_recv.at[kind, b], peer)

    def c_copy(b, kind, col, parts, row):
        ref = tile(b, row, col, parts)
        return remote(ref, ref, c_send.at[kind, b], c_recv.at[kind, b], to_core)

    c_kinds = ((0, x, both), (1, left, both), (2, right, both), (3, far, half0), (4, far, half1))

    z_order, late = [0, 1], list(range(first0, nb))
    for b in range(2, first0):
        z_order.append(b)
        if late:
            z_order.append(late.pop(0))
    z_order += late
    w_copy = remote(weight, weigh, w_sems.at[0], w_sems.at[1], to_z)
    w_copy.start()

    def pack_copy(b):
        kind, row, col = order[b]
        source = factor.at[0, :, row, col] if kind == "L" else dinv.at[0, :, row]
        return pltpu.make_async_copy(source, pack.at[b], pack_sem.at[b])

    def masked(b):
        kind, row, col = order[b]
        if kind == "L":
            per_block = tiles.shape[1] // nsup
            here = per_block // 2
            size = rows // here

            @pl.loop(0, 2 * here)
            def _(i):
                q, t = i // here, lax.rem(i, here)
                keep = tiles[col, row * per_block + zh * here + t].astype(jnp.float32)
                lines = pl.ds(pl.multiple_of(t * size, size), size)
                pack[b, q, lines, :] = pack[b, q, lines, :] * keep

    for b in z_order:
        pack_copy(b).start()
    for b in z_order:
        pack_copy(b).wait()
        masked(b)
        z_copy(b, zh).start()

    def own_part(b):
        z_copy(b, core).wait_recv()
        c_copy(b, 0, x, both, core).start()

    def own(b):
        if b < first0:
            own_part(b)
        x_copy(b, 0, x, both, to_right).start()
        x_copy(b, 1, x, both, to_left).start()

    def pass_on(b):
        x_copy(b, 0, left, both, to_right).wait_recv()
        x_copy(b, 2, left, half0, to_right).start()
        c_copy(b, 1, left, both, core).start()
        x_copy(b, 1, right, both, to_left).wait_recv()
        x_copy(b, 3, right, half1, to_left).start()
        c_copy(b, 2, right, both, core).start()

    def finish(b):
        x_copy(b, 2, far, half0, to_right).wait_recv()
        c_copy(b, 3, far, half0, core).start()
        x_copy(b, 3, far, half1, to_left).wait_recv()
        c_copy(b, 4, far, half1, core).start()

    ahead, delay, pace = 2, 4, 5

    sym0 = where[("D", nsup - 1, nsup - 1)]
    syms = range(sym0, first0)

    def piece(b, row, col, part=None, start=0, size=None):
        return full.at[
            b,
            pl.ds(core if part is None else part, 1),
            pl.ds(pl.multiple_of(row * cols + start, cols // 2), size or cols),
            pl.ds(pl.multiple_of(col * cols, cols), cols),
        ]

    def dx_copy(b, kind, row, col, peer, start=0, size=None):
        ref = piece(b, row, col, None, start, size)
        return remote(ref, ref, dx_send.at[kind, b - sym0], dx_recv.at[kind, b - sym0], peer)

    def dc_copy(b, kind, row, col, part, start=0, size=None):
        ref = piece(b, row, col, part, start, size)
        return remote(ref, ref, dc_send.at[kind, b - sym0], dc_recv.at[kind, b - sym0], to_core)

    part_size = cols // 2
    out_right = ((0, x), (1, far), (2, left))
    out_left = ((3, x), (4, right))
    in_left = ((0, left), (1, right), (2, far))
    in_right = ((3, right), (4, far))
    dc_kinds = (
        (0, left, left, 0, cols), (1, right, left, 0, cols), (2, far, left, 0, cols),
        (3, right, right, 0, cols), (4, far, right, 0, cols),
        (5, far, far, 0, part_size), (6, far, far, part_size, part_size),
    )

    def own_sym(b):
        c_copy(b, 0, x, both, 1 - core).wait_recv()
        for kind, row in out_right:
            dx_copy(b, kind, row, x, to_right).start()
        for kind, row in out_left:
            dx_copy(b, kind, row, x, to_left).start()

    def pass_sym(b):
        for kind, row in in_left:
            dx_copy(b, kind, row, left, to_right).wait_recv()
            if kind == 0:
                dx_copy(b, 5, left, left, to_right, 0, part_size).start()
            dc_copy(b, kind, row, left, core).start()
        for kind, row in in_right:
            dx_copy(b, kind, row, right, to_left).wait_recv()
            if kind == 3:
                dx_copy(b, 6, right, right, to_left, part_size, part_size).start()
            dc_copy(b, kind, row, right, core).start()

    def finish_sym(b):
        dx_copy(b, 5, far, far, to_right, 0, part_size).wait_recv()
        dc_copy(b, 5, far, far, core, 0, part_size).start()
        dx_copy(b, 6, far, far, to_left, part_size, part_size).wait_recv()
        dc_copy(b, 6, far, far, core, part_size, part_size).start()

    def fill(slot):
        def place_of(q, row, col):
            return (
                slot,
                q,
                pl.ds(pl.multiple_of(row * cols, cols), cols),
                pl.ds(pl.multiple_of(col * cols, cols), cols),
            )

        @pl.loop(0, 2)
        def _(q):
            for row, col in ((left, x), (right, x), (far, x), (right, left), (far, left), (far, right)):
                blk[place_of(q, col, row)] = jnp.transpose(blk[place_of(q, row, col)])

    def service(s):
        if s + ahead + 2 in syms:
            own_part(s + ahead + 2)
        if s + ahead < last:
            (own_sym if s + ahead in syms else own)(s + ahead)
        if 1 <= s and first0 + s - 1 <= last:
            own_part(first0 + s - 1)
        if s < last:
            (pass_sym if s in syms else pass_on)(s)
        if ahead <= s < last + ahead:
            (finish_sym if s - ahead in syms else finish)(s - ahead)

    def arrived(b):
        if b in syms:
            for kind, row, col, start, size in dc_kinds:
                dc_copy(b, kind, row, col, 1 - core, start, size).wait_recv()
            return
        for kind, col, parts in c_kinds:
            if kind > 0 or b < first0:
                c_copy(b, kind, col, parts, 1 - core).wait_recv()

    def blk_copy(b, slot):
        return pltpu.make_async_copy(full.at[b], blk.at[slot], blk_sem.at[slot])

    def unit_rows(index):
        return pl.ds(pl.multiple_of(index * unit, unit), unit)

    def own_copy(i):
        columns = pl.ds(pl.multiple_of(x * cols, cols), cols)
        return pltpu.make_async_copy(full.at[first0 + i, :, :, columns], own_cols.at[i], own_sem.at[i])

    def set_first(acc, index, i):
        lane = lax.broadcasted_iota(jnp.int32, (n, cols), 1)
        line = lax.broadcasted_iota(jnp.int32, (n, cols), 0)
        pick = jnp.where(lane == line + core * n, 1.0, 0.0).astype(jnp.bfloat16)
        for q in range(2):
            high, low = split(own_cols[i, q])
            acc[0, pl.ds(index * unit + q * n, n), :] = dot(pick, high, 1) + dot(pick, low, 1)
        acc[1, pl.ds(index * unit, unit), :] = jnp.zeros((unit, width), jnp.float32)

    def begin():
        for i in range(nsup):
            c_copy(first0 + i, 0, x, both, 1 - core).wait_recv()
            own_copy(i).start()
        for i in range(nsup):
            own_copy(i).wait()
        for row in range(1, nsup):
            set_first(acc_z, tri(row - 1), row - 1)
        finish_z(1)

    def joined(acc, index):
        p, q = acc[0, unit_rows(index), :], acc[1, unit_rows(index), :]
        return p[:n] - q[n:], p[n:] + q[:n]

    def finish_z(row):
        @pl.loop(0, row)
        def _(k):
            re, im = joined(acc_z, tri(row - 1) + k)
            high, low = split(-jnp.concatenate([re, im], axis=0))
            z_high[unit_rows(tri(row) + k), :] = high
            z_low[unit_rows(tri(row) + k), :] = low

        lane = lax.broadcasted_iota(jnp.int32, (unit, width), 1)
        line = lax.broadcasted_iota(jnp.int32, (unit, width), 0)
        hit = (lane == line + x * cols + core * n) & (line < n)
        z_high[pl.ds((tri(row) + row) * unit, unit), :] = jnp.where(hit, 1.0, 0.0).astype(jnp.bfloat16)
        z_low[pl.ds((tri(row) + row) * unit, unit), :] = jnp.zeros((unit, width), jnp.bfloat16)

    def multiply(acc, acc_at, high, low, at, units, slot, transposed, fresh):
        m, kept = units * unit, (units - fresh) * unit
        here = pl.ds(at * unit, m)

        @pl.loop(0, 2)
        def _(q):
            right_high, right_low = split(blk[slot, q])
            dim = 1 if transposed else 0
            upper = high[here, :]
            total = dot(jnp.concatenate([upper, low[here, :]], axis=0), right_high, dim)
            total = total[:m] + total[m:] + dot(upper, right_low, dim)
            if kept:
                acc[q, pl.ds(acc_at * unit, kept), :] += total[:kept]
            if fresh:
                acc[q, pl.ds(acc_at * unit + kept, fresh * unit), :] = total[kept:]

    def forward(row, mid, slot):
        multiply(acc_z, tri(row - 1), z_high, z_low, tri(mid), mid + 1, slot, True, 1)
        if row == nsup - 1:
            finish_z(mid + 1)

    def backward(row, low_row, slot):
        if low_row == row:
            fill(slot)
            multiply(acc_g, 0, z_high, z_low, tri(row), row + 1, slot, False, row + 1)
        else:
            multiply(acc_g, 0, g_high, g_low, tri(low_row), row + 1, slot, False, 0)

    def finish_g(row):
        w_re, w_im = weigh[0:1, :], weigh[1:2, :]

        @pl.loop(0, row + 1)
        def _(k):
            re, im = joined(acc_g, k)
            real[off(nsup, row) + k] = (w_re * re - w_im * im).reshape(real.shape[1:])
            if row > 0:
                high, low = split(-jnp.concatenate([re, im], axis=0))
                g_high[unit_rows(tri(row) + k), :] = high
                g_low[unit_rows(tri(row) + k), :] = low

        for copy in first_stage(row):
            copy.start()

    def first_stage(row):
        span = pl.ds(off(nsup, row), row + 1)
        copies = []
        for d, (h, l) in enumerate(z_peers):
            lanes = pl.ds(pl.multiple_of(h * half_w, half_w), half_w)
            copies.append(
                remote(
                    real.at[span, :, l, :, lanes], part1.at[d, span], r_send.at[0, row, d], r_recv.at[0, row, d],
                    {"zh": h, "zl": l},
                )
            )
        return copies

    def second_stage(row):
        span = pl.ds(off(nsup, row), row + 1)
        copies = []
        for d, (p, q) in enumerate(y_peers):
            lanes = pl.ds(pl.multiple_of(p * cols, cols), cols)
            copies.append(
                remote(
                    sum1.at[span, q, :, lanes], part2.at[d, span], r_send.at[1, row, d], r_recv.at[1, row, d],
                    {"a": p, "b": q},
                )
            )
        return copies

    def reduce_first(row):
        for copy in first_stage(row):
            copy.wait_recv()
        span = pl.ds(off(nsup, row), row + 1)
        lanes = pl.ds(pl.multiple_of(zh * half_w, half_w), half_w)
        sum1[span] = real[span, :, zl, :, lanes] + part1[0, span] + part1[1, span] + part1[2, span]
        for copy in second_stage(row):
            copy.start()

    def reduce_second(row):
        for copy in second_stage(row):
            copy.wait_recv()
        span = pl.ds(off(nsup, row), row + 1)
        lanes = pl.ds(pl.multiple_of(a_ * cols, cols), cols)
        share[span] = sum1[span, b_, :, lanes] + part2[0, span] + part2[1, span] + part2[2, span]
        if row > 0:

            @pl.when(moves)
            def _():
                mirror_copy(row).start()

        if row == 2:
            start_low(0)
            start_low(1)
        if row == 0:
            start_low(2)

    def mirror_copy(row):
        span = pl.ds(off(nsup, row), row)
        return remote(
            share.at[span], mirror.at[span], m_send.at[row], m_recv.at[row], dict(zip(AXES, goes_to))
        )

    def low_copies(g):
        copies = []
        for d, (i, j, k) in enumerate(l_peers):
            lines = pl.ds(pl.multiple_of((4 * i + 2 * j + k) * 16, 16), 16)
            copies.append(
                remote(
                    low_from.at[g, lines], low_to.at[g, place], l_send.at[g, d], l_recv.at[g, d],
                    {"b": i, "zl": j, "core": k},
                )
            )
        return copies

    def start_low(g):
        low_from[g] = jnp.transpose(share[pl.ds(8 * g, 8)].reshape(cols, cols))
        low_to[g, place] = low_from[g, pl.ds(pl.multiple_of(place * 16, 16), 16), :]
        for copy in low_copies(g):
            copy.start()

    def finish_low(g):
        for copy in low_copies(g):
            copy.wait_recv()
        places = [4 * j + 2 * k + i for i in range(2) for j in range(2) for k in range(2)]
        for row in range(nsup):
            for col in range(row + 1):
                p = off(nsup, row) + col - 8 * g
                if 0 <= p < 8:
                    pieces = [low_to[g, s, :, p * 16 : p * 16 + 16] for s in places]
                    out[row, col] = jnp.concatenate(pieces, axis=1)

    def finish_mirror():
        @pl.when(moves)
        def _():
            for row in range(1, nsup):
                mirror_copy(row).wait_recv()

        @pl.when(stays)
        def _():
            mirror[...] = share[pl.ds(0, tri(nsup))]

        for row in range(1, nsup):
            for col in range(row):
                out[col, row] = mirror[off(nsup, row) + col]


    items = []
    for b in range(nsup * (nsup - 1) // 2 - (nsup - 1)):
        kind, row, mid = order[b]
        items.append((functools.partial(forward, row, mid), b, b, mid))
    for row in range(nsup - 1, 0, -1):
        items.append((functools.partial(backward, row, row), where[("D", row, row)], where[("D", row, row)], row + 1))
        for low_row in range(row + 1, nsup):
            items.append(
                (functools.partial(backward, row, low_row), where[("L", low_row, row)], where[("D", row, row)], row + 1)
            )
    for low_row in range(1, nsup):
        b = where[("L", low_row, 0)]
        items.append((functools.partial(backward, 0, low_row), b, b, 1))

    for i in range(24 - tri(nsup)):
        share[tri(nsup) + i] = jnp.zeros(share.shape[1:], jnp.float32)
    for b in range(ahead):
        own(b)
    state = {"done": -1, "loaded": -1}
    seen = set()

    def fetch(i):
        if i <= state["loaded"] or i >= len(items) or items[i][2] + ahead > state["done"]:
            return
        b = items[i][1]
        if b not in seen:
            seen.add(b)
            arrived(b)
        blk_copy(b, i % 2).start()
        state["loaded"] = i

    todo, started, summed = 0, [], []
    ready_at = first0 - where[("L", 1, 0)] + nsup + 1
    finals = {}
    for i, (fn, b, avail, units) in enumerate(items):
        if fn.func is backward and fn.args[1] == nsup - 1:
            finals[i] = fn.args[0]
    for s in range(last + ahead):
        service(s)
        state["done"] = s
        if s == ready_at:
            begin()
        if s < ready_at:
            continue
        for row, since in list(summed):
            if s >= since + delay:
                reduce_second(row)
                summed.remove((row, since))
        for row, since in list(started):
            if s >= since + delay:
                reduce_first(row)
                started.remove((row, since))
                summed.append((row, s))
        budget = pace if s < last + ahead - 1 else 10**6
        while todo < len(items) and items[todo][2] + ahead <= s and budget > 0:
            fetch(todo)
            fetch(todo + 1)
            blk_copy(items[todo][1], todo % 2).wait()
            if todo == len(items) - nsup + 1:
                set_first(acc_g, 0, nsup - 1)
            items[todo][0](todo % 2)
            budget -= items[todo][3]
            if todo in finals:
                if finals[todo] == nsup - 1:
                    w_copy.wait_recv()
                finish_g(finals[todo])
                started.append((finals[todo], s))
            todo += 1
    for row, since in started:
        reduce_first(row)
    for row, since in summed + started:
        reduce_second(row)
    for g in range(3):
        finish_low(g)
    finish_mirror()

    w_copy.wait_send()
    for g in range(3):
        for copy in low_copies(g):
            copy.wait_send()

    @pl.when(moves)
    def _():
        for row in range(1, nsup):
            mirror_copy(row).wait_send()

    for b in range(nb):
        z_copy(b, zh).wait_send()
        c_copy(b, 0, x, both, core).wait_send()
        if b in syms:
            for kind, row in out_right + out_left:
                dx_copy(b, kind, row, x, to_right).wait_send()
            dx_copy(b, 5, left, left, to_right, 0, part_size).wait_send()
            dx_copy(b, 6, right, right, to_left, part_size, part_size).wait_send()
            for kind, row, col, start, size in dc_kinds:
                dc_copy(b, kind, row, col, core, start, size).wait_send()
        elif b < last:
            x_copy(b, 0, x, both, to_right).wait_send()
            x_copy(b, 1, x, both, to_left).wait_send()
            x_copy(b, 2, left, half0, to_right).wait_send()
            x_copy(b, 3, right, half1, to_left).wait_send()
            for kind, col, parts in c_kinds[1:]:
                c_copy(b, kind, col, parts, core).wait_send()
    for row in range(nsup):
        for copy in first_stage(row) + second_stage(row):
            copy.wait_send()


def window_share(factor, dinv, tiles, weight, ncol):
    _, parts, nsup, _, rows, cols = factor.shape
    nb = tri(nsup)
    width, unit, pairs = 2 * rows, cols, tri(nsup)
    sems = pltpu.SemaphoreType.DMA
    f32, bf16 = jnp.float32, jnp.bfloat16
    return pl.pallas_call(
        functools.partial(window_kernel, nsup),
        out_shape=(
            jax.ShapeDtypeStruct((nb, parts, width, width), f32),
            jax.ShapeDtypeStruct((nsup, nsup, 16, cols), f32),
        ),
        in_specs=[
            pl.BlockSpec(memory_space=pl.ANY),
            pl.BlockSpec(memory_space=pl.ANY),
            pl.BlockSpec(memory_space=pltpu.SMEM),
            pl.BlockSpec(memory_space=pltpu.VMEM),
        ],
        out_specs=(pl.BlockSpec(memory_space=pl.ANY), pl.BlockSpec(memory_space=pltpu.VMEM)),
        scratch_shapes=[
            pltpu.VMEM((nb, parts, rows, cols), f32),
            pltpu.VMEM(weight.shape, f32),
            pltpu.VMEM((2, parts, width, width), f32),
            pltpu.VMEM((nsup, parts, width, cols), f32),
            pltpu.VMEM((2, tri(nsup - 1) * unit, width), f32),
            pltpu.VMEM((2, nsup * unit, width), f32),
            pltpu.VMEM((pairs * unit, width), bf16),
            pltpu.VMEM((pairs * unit, width), bf16),
            pltpu.VMEM((pairs * unit, width), bf16),
            pltpu.VMEM((pairs * unit, width), bf16),
            pltpu.VMEM((pairs, 2, 2, 16, width), f32),
            pltpu.VMEM((3, pairs, 2, 16, width // 2), f32),
            pltpu.VMEM((pairs, 2, 16, width // 2), f32),
            pltpu.VMEM((3, pairs, 16, cols), f32),
            pltpu.VMEM((24, 16, cols), f32),
            pltpu.VMEM((pairs, 16, cols), f32),
            pltpu.VMEM((3, cols, cols), f32),
            pltpu.VMEM((3, 8, 16, cols), f32),
            sems((nb,)), sems((nb,)), sems((4, nb)), sems((4, nb)), sems((5, nb)), sems((5, nb)),
            sems((2, nsup, 3)), sems((2, nsup, 3)), sems((nsup,)), sems((nsup,)), sems((3, 7)), sems((3, 7)), sems((2,)),
            *[sems((7, nsup - 1)) for _ in range(4)], sems((2,)), sems((nsup,)), sems((nb,)),
        ],
        compiler_params=pltpu.CompilerParams(
            collective_id=0, has_side_effects=True, vmem_limit_bytes=60 * 1024 * 1024
        ),
    )(factor, dinv, tiles, weight)[1]


def on_device(l_factor, dinv, weights, tiles):
    width = 2 * l_factor.shape[3]
    weight = jnp.broadcast_to(jnp.pad(weights[0], (0, 6))[:, None], (8, width))
    factor = jnp.swapaxes(l_factor, 3, 4)
    blocks = window_share(factor, dinv, tiles, weight, lax.axis_size("x"))
    return jnp.transpose(blocks, (0, 2, 1, 3))[:, None]


def solution(mesh):
    fine = Mesh(mesh.devices.reshape(2, 2, 2, 2, 2, 4), AXES)
    pole = ("a", "b", "zl", "core")
    return jax.shard_map(
        on_device,
        mesh=fine,
        in_specs=(P(pole, None, None, "zh", None, "x"), P(pole, None, None, "zh", "x"), P(pole, None), P()),
        out_specs=P(None, "zh", pole, None, "x"),
        check_vma=False,
    )
```

```python
import functools

import jax
import jax.numpy as jnp
from jax import lax
from jax.experimental import pallas as pl
from jax.experimental.pallas import tpu as pltpu
from jax.sharding import Mesh
from jax.sharding import PartitionSpec as P

AXES = ("a", "b", "zl", "core", "zh", "x")
MESH = pl.DeviceIdType.MESH


def block_order(nsup):
    lower = [("L", row, col) for col in range(1, nsup - 1) for row in range(col + 1, nsup)]
    diag = [("D", col, col) for col in range(nsup - 1, 0, -1)]
    first = [("L", row, 0) for row in range(1, nsup)]
    return lower + diag + first + [("D", 0, 0)]


def tri(row):
    return row * (row + 1) // 2


def off(nsup, row):
    return tri(nsup) - tri(row + 1)


def split(value):
    high = value.astype(jnp.bfloat16)
    return high, (value - high.astype(jnp.float32)).astype(jnp.bfloat16)


def dot(a, b, dim):
    return lax.dot_general(a, b, (((1,), (dim,)), ((), ())), preferred_element_type=jnp.float32)


def window_kernel(
    nsup, factor, dinv, tiles, weight, full, out,
    pack, weigh, blk, own_cols, acc_z, acc_g, z_high, z_low, g_high, g_low, real, part1, sum1, part2, share, mirror,
    low_from, low_to,
    z_send, z_recv, x_send, x_recv, c_send, c_recv, r_send, r_recv, m_send, m_recv, l_send, l_recv, w_sems,
    dx_send, dx_recv, dc_send, dc_recv, blk_sem, own_sem, pack_sem,
):
    order = block_order(nsup)
    where = {item: i for i, item in enumerate(order)}
    nb = len(order)
    last = nb - 1
    first0 = where[("L", 1, 0)]
    a_, b_, zl, core, zh, x = (lax.axis_index(n) for n in AXES)
    ncol = lax.axis_size("x")
    rows, cols = pack.shape[2], pack.shape[3]
    width = full.shape[2]
    half_w = width // 2
    n = cols // 2
    unit = 2 * n
    right, left, far = lax.rem(x + 1, ncol), lax.rem(x + ncol - 1, ncol), lax.rem(x + 2, ncol)
    to_z = {"zl": 1 - zl, "core": zh, "zh": core}
    to_right, to_left, to_core = {"x": right}, {"x": left}, {"core": 1 - core}

    def other(value, flag):
        return 1 - value if flag else value

    z_peers = [(other(zh, d >> 1), other(zl, d & 1)) for d in (1, 2, 3)]
    y_peers = [(other(a_, d >> 1), other(b_, d & 1)) for d in (1, 2, 3)]
    barrier = pltpu.get_barrier_semaphore()
    peers = [to_z, to_right, to_left, to_core]
    peers += [{"zh": h, "zl": l} for h, l in z_peers] + [{"a": p, "b": q} for p, q in y_peers]
    l_peers = [(other(b_, d >> 2), other(zl, (d >> 1) & 1), other(core, d & 1)) for d in range(1, 8)]
    peers += [{"b": i, "zl": j, "core": k} for i, j, k in l_peers]
    place = 4 * b_ + 2 * zl + core
    goes_to = (lax.rem(x, 2), core, b_, zl, x // 2, zh * 2 + a_)
    comes_from = (lax.rem(x, 2), zl, core, b_, x // 2, zh * 2 + a_)
    stays = (a_ == goes_to[0]) & (b_ == core) & (zl == b_) & (zh == goes_to[4]) & (x == goes_to[5])
    moves = jnp.logical_not(stays)
    peers += [dict(zip(AXES, goes_to)), dict(zip(AXES, comes_from))]
    for peer in peers:
        pl.semaphore_signal(barrier, inc=1, device_id=peer, device_id_type=MESH)

    pl.semaphore_wait(barrier, len(peers))

    both, half0, half1 = pl.ds(0, 2), pl.ds(0, 1), pl.ds(1, 1)

    def tile(b, row, col, parts=both):
        return full.at[
            b,
            parts,
            pl.ds(pl.multiple_of(row * rows, rows), rows),
            pl.ds(pl.multiple_of(col * cols, cols), cols),
        ]

    def remote(src, dst, send, recv, peer):
        return pltpu.make_async_remote_copy(src, dst, send, recv, device_id=peer, device_id_type=MESH)

    def z_copy(b, row):
        return remote(pack.at[b], tile(b, row, x), z_send.at[b], z_recv.at[b], to_z)

    def x_copy(b, kind, col, parts, peer):
        ref = tile(b, core, col, parts)
        return remote(ref, ref, x_send.at[kind, b], x_recv.at[kind, b], peer)

    def c_copy(b, kind, col, parts, row):
        ref = tile(b, row, col, parts)
        return remote(ref, ref, c_send.at[kind, b], c_recv.at[kind, b], to_core)

    c_kinds = ((0, x, both), (1, left, both), (2, right, both), (3, far, half0), (4, far, half1))

    z_order, late = [0, 1], list(range(first0, nb))
    for b in range(2, first0):
        z_order.append(b)
        if late:
            z_order.append(late.pop(0))
    z_order += late
    w_copy = remote(weight, weigh, w_sems.at[0], w_sems.at[1], to_z)
    w_copy.start()

    def pack_copy(b):
        kind, row, col = order[b]
        source = factor.at[0, :, row, col] if kind == "L" else dinv.at[0, :, row]
        return pltpu.make_async_copy(source, pack.at[b], pack_sem.at[b])

    def masked(b):
        kind, row, col = order[b]
        if kind == "L":
            per_block = tiles.shape[1] // nsup
            here = per_block // 2
            size = rows // here

            @pl.loop(0, 2 * here)
            def _(i):
                q, t = i // here, lax.rem(i, here)
                keep = tiles[col, row * per_block + zh * here + t].astype(jnp.float32)
                lines = pl.ds(pl.multiple_of(t * size, size), size)
                pack[b, q, lines, :] = pack[b, q, lines, :] * keep

    for b in z_order:
        pack_copy(b).start()
    for b in z_order:
        pack_copy(b).wait()
        masked(b)
        z_copy(b, zh).start()

    def own_part(b):
        z_copy(b, core).wait_recv()
        c_copy(b, 0, x, both, core).start()

    def own(b):
        if b < first0:
            own_part(b)
        x_copy(b, 0, x, both, to_right).start()
        x_copy(b, 1, x, both, to_left).start()

    def pass_on(b):
        x_copy(b, 0, left, both, to_right).wait_recv()
        x_copy(b, 2, left, half0, to_right).start()
        c_copy(b, 1, left, both, core).start()
        x_copy(b, 1, right, both, to_left).wait_recv()
        x_copy(b, 3, right, half1, to_left).start()
        c_copy(b, 2, right, both, core).start()

    def finish(b):
        x_copy(b, 2, far, half0, to_right).wait_recv()
        c_copy(b, 3, far, half0, core).start()
        x_copy(b, 3, far, half1, to_left).wait_recv()
        c_copy(b, 4, far, half1, core).start()

    ahead, delay, pace, early = 3, 4, 5, 12

    sym0 = where[("D", nsup - 1, nsup - 1)]
    syms = range(sym0, first0)

    def piece(b, row, col, part=None, start=0, size=None):
        return full.at[
            b,
            pl.ds(core if part is None else part, 1),
            pl.ds(pl.multiple_of(row * cols + start, cols // 2), size or cols),
            pl.ds(pl.multiple_of(col * cols, cols), cols),
        ]

    def dx_copy(b, kind, row, col, peer, start=0, size=None):
        ref = piece(b, row, col, None, start, size)
        return remote(ref, ref, dx_send.at[kind, b - sym0], dx_recv.at[kind, b - sym0], peer)

    def dc_copy(b, kind, row, col, part, start=0, size=None):
        ref = piece(b, row, col, part, start, size)
        return remote(ref, ref, dc_send.at[kind, b - sym0], dc_recv.at[kind, b - sym0], to_core)

    part_size = cols // 2
    out_right = ((0, x), (1, far), (2, left))
    out_left = ((3, x), (4, right))
    in_left = ((0, left), (1, right), (2, far))
    in_right = ((3, right), (4, far))
    dc_kinds = (
        (0, left, left, 0, cols), (1, right, left, 0, cols), (2, far, left, 0, cols),
        (3, right, right, 0, cols), (4, far, right, 0, cols),
        (5, far, far, 0, part_size), (6, far, far, part_size, part_size),
    )

    def own_sym(b):
        c_copy(b, 0, x, both, 1 - core).wait_recv()
        for kind, row in out_right:
            dx_copy(b, kind, row, x, to_right).start()
        for kind, row in out_left:
            dx_copy(b, kind, row, x, to_left).start()

    def pass_sym(b):
        for kind, row in in_left:
            dx_copy(b, kind, row, left, to_right).wait_recv()
            if kind == 0:
                dx_copy(b, 5, left, left, to_right, 0, part_size).start()
            dc_copy(b, kind, row, left, core).start()
        for kind, row in in_right:
            dx_copy(b, kind, row, right, to_left).wait_recv()
            if kind == 3:
                dx_copy(b, 6, right, right, to_left, part_size, part_size).start()
            dc_copy(b, kind, row, right, core).start()

    def finish_sym(b):
        dx_copy(b, 5, far, far, to_right, 0, part_size).wait_recv()
        dc_copy(b, 5, far, far, core, 0, part_size).start()
        dx_copy(b, 6, far, far, to_left, part_size, part_size).wait_recv()
        dc_copy(b, 6, far, far, core, part_size, part_size).start()

    def fill(slot):
        def place_of(q, row, col):
            return (
                slot,
                q,
                pl.ds(pl.multiple_of(row * cols, cols), cols),
                pl.ds(pl.multiple_of(col * cols, cols), cols),
            )

        @pl.loop(0, 2)
        def _(q):
            for row, col in ((left, x), (right, x), (far, x), (right, left), (far, left), (far, right)):
                blk[place_of(q, col, row)] = jnp.transpose(blk[place_of(q, row, col)])

    def service(s):
        if s + ahead + 2 in syms:
            own_part(s + ahead + 2)
        if s + ahead < last:
            (own_sym if s + ahead in syms else own)(s + ahead)
        if 1 <= s and first0 + s - 1 <= last:
            own_part(first0 + s - 1)
        if s < last:
            (pass_sym if s in syms else pass_on)(s)
        if ahead <= s < last + ahead:
            (finish_sym if s - ahead in syms else finish)(s - ahead)

    def arrived(b):
        if b in syms:
            for kind, row, col, start, size in dc_kinds:
                dc_copy(b, kind, row, col, 1 - core, start, size).wait_recv()
            return
        for kind, col, parts in c_kinds:
            if kind > 0 or b < first0:
                c_copy(b, kind, col, parts, 1 - core).wait_recv()

    def blk_copy(b, slot):
        return pltpu.make_async_copy(full.at[b], blk.at[slot], blk_sem.at[slot])

    def unit_rows(index):
        return pl.ds(pl.multiple_of(index * unit, unit), unit)

    def own_copy(i):
        columns = pl.ds(pl.multiple_of(x * cols, cols), cols)
        return pltpu.make_async_copy(full.at[first0 + i, :, :, columns], own_cols.at[i], own_sem.at[i])

    def set_first(acc, index, i):
        lane = lax.broadcasted_iota(jnp.int32, (n, cols), 1)
        line = lax.broadcasted_iota(jnp.int32, (n, cols), 0)
        pick = jnp.where(lane == line + core * n, 1.0, 0.0).astype(jnp.bfloat16)
        for q in range(2):
            high, low = split(own_cols[i, q])
            acc[0, pl.ds(index * unit + q * n, n), :] = dot(pick, high, 1) + dot(pick, low, 1)
        acc[1, pl.ds(index * unit, unit), :] = jnp.zeros((unit, width), jnp.float32)

    def begin():
        for i in range(nsup):
            c_copy(first0 + i, 0, x, both, 1 - core).wait_recv()
            own_copy(i).start()
        for i in range(nsup):
            own_copy(i).wait()
        for row in range(1, nsup):
            set_first(acc_z, tri(row - 1), row - 1)
        finish_z(1)

    def joined(acc, index):
        p, q = acc[0, unit_rows(index), :], acc[1, unit_rows(index), :]
        return p[:n] - q[n:], p[n:] + q[:n]

    def finish_z(row):
        @pl.loop(0, row)
        def _(k):
            re, im = joined(acc_z, tri(row - 1) + k)
            high, low = split(-jnp.concatenate([re, im], axis=0))
            z_high[unit_rows(tri(row) + k), :] = high
            z_low[unit_rows(tri(row) + k), :] = low

        lane = lax.broadcasted_iota(jnp.int32, (unit, width), 1)
        line = lax.broadcasted_iota(jnp.int32, (unit, width), 0)
        hit = (lane == line + x * cols + core * n) & (line < n)
        z_high[pl.ds((tri(row) + row) * unit, unit), :] = jnp.where(hit, 1.0, 0.0).astype(jnp.bfloat16)
        z_low[pl.ds((tri(row) + row) * unit, unit), :] = jnp.zeros((unit, width), jnp.bfloat16)

    def multiply(acc, acc_at, high, low, at, units, slot, transposed, fresh):
        m, kept = units * unit, (units - fresh) * unit
        here = pl.ds(at * unit, m)

        @pl.loop(0, 2)
        def _(q):
            right_high, right_low = split(blk[slot, q])
            dim = 1 if transposed else 0
            upper = high[here, :]
            total = dot(jnp.concatenate([upper, low[here, :]], axis=0), right_high, dim)
            total = total[:m] + total[m:] + dot(upper, right_low, dim)
            if kept:
                acc[q, pl.ds(acc_at * unit, kept), :] += total[:kept]
            if fresh:
                acc[q, pl.ds(acc_at * unit + kept, fresh * unit), :] = total[kept:]

    def forward(row, mid, slot):
        multiply(acc_z, tri(row - 1), z_high, z_low, tri(mid), mid + 1, slot, True, 1)
        if row == nsup - 1:
            finish_z(mid + 1)

    def backward(row, low_row, slot):
        if low_row == row:
            fill(slot)
            multiply(acc_g, 0, z_high, z_low, tri(row), row + 1, slot, False, row + 1)
        else:
            multiply(acc_g, 0, g_high, g_low, tri(low_row), row + 1, slot, False, 0)

    def finish_g(row):
        w_re, w_im = weigh[0:1, :], weigh[1:2, :]

        @pl.loop(0, row + 1)
        def _(k):
            re, im = joined(acc_g, k)
            real[off(nsup, row) + k] = (w_re * re - w_im * im).reshape(real.shape[1:])
            if row > 0:
                high, low = split(-jnp.concatenate([re, im], axis=0))
                g_high[unit_rows(tri(row) + k), :] = high
                g_low[unit_rows(tri(row) + k), :] = low

        for copy in first_stage(row):
            copy.start()

    def first_stage(row):
        span = pl.ds(off(nsup, row), row + 1)
        copies = []
        for d, (h, l) in enumerate(z_peers):
            lanes = pl.ds(pl.multiple_of(h * half_w, half_w), half_w)
            copies.append(
                remote(
                    real.at[span, :, l, :, lanes], part1.at[d, span], r_send.at[0, row, d], r_recv.at[0, row, d],
                    {"zh": h, "zl": l},
                )
            )
        return copies

    def second_stage(row):
        span = pl.ds(off(nsup, row), row + 1)
        copies = []
        for d, (p, q) in enumerate(y_peers):
            lanes = pl.ds(pl.multiple_of(p * cols, cols), cols)
            copies.append(
                remote(
                    sum1.at[span, q, :, lanes], part2.at[d, span], r_send.at[1, row, d], r_recv.at[1, row, d],
                    {"a": p, "b": q},
                )
            )
        return copies

    def reduce_first(row):
        for copy in first_stage(row):
            copy.wait_recv()
        span = pl.ds(off(nsup, row), row + 1)
        lanes = pl.ds(pl.multiple_of(zh * half_w, half_w), half_w)
        sum1[span] = real[span, :, zl, :, lanes] + part1[0, span] + part1[1, span] + part1[2, span]
        for copy in second_stage(row):
            copy.start()

    def reduce_second(row):
        for copy in second_stage(row):
            copy.wait_recv()
        span = pl.ds(off(nsup, row), row + 1)
        lanes = pl.ds(pl.multiple_of(a_ * cols, cols), cols)
        share[span] = sum1[span, b_, :, lanes] + part2[0, span] + part2[1, span] + part2[2, span]
        if row > 0:

            @pl.when(moves)
            def _():
                mirror_copy(row).start()

        if row == 2:
            start_low(0)
            start_low(1)
        if row == 0:
            start_low(2)

    def mirror_copy(row):
        span = pl.ds(off(nsup, row), row)
        return remote(
            share.at[span], mirror.at[span], m_send.at[row], m_recv.at[row], dict(zip(AXES, goes_to))
        )

    def low_copies(g):
        copies = []
        for d, (i, j, k) in enumerate(l_peers):
            lines = pl.ds(pl.multiple_of((4 * i + 2 * j + k) * 16, 16), 16)
            copies.append(
                remote(
                    low_from.at[g, lines], low_to.at[g, place], l_send.at[g, d], l_recv.at[g, d],
                    {"b": i, "zl": j, "core": k},
                )
            )
        return copies

    def start_low(g):
        low_from[g] = jnp.transpose(share[pl.ds(8 * g, 8)].reshape(cols, cols))
        low_to[g, place] = low_from[g, pl.ds(pl.multiple_of(place * 16, 16), 16), :]
        for copy in low_copies(g):
            copy.start()

    def finish_low(g):
        for copy in low_copies(g):
            copy.wait_recv()
        places = [4 * j + 2 * k + i for i in range(2) for j in range(2) for k in range(2)]
        for row in range(nsup):
            for col in range(row + 1):
                p = off(nsup, row) + col - 8 * g
                if 0 <= p < 8:
                    pieces = [low_to[g, s, :, p * 16 : p * 16 + 16] for s in places]
                    out[row, col] = jnp.concatenate(pieces, axis=1)

    def finish_mirror():
        @pl.when(moves)
        def _():
            for row in range(1, nsup):
                mirror_copy(row).wait_recv()

        @pl.when(stays)
        def _():
            mirror[...] = share[pl.ds(0, tri(nsup))]

        for row in range(1, nsup):
            for col in range(row):
                out[col, row] = mirror[off(nsup, row) + col]


    items = []
    for b in range(nsup * (nsup - 1) // 2 - (nsup - 1)):
        kind, row, mid = order[b]
        items.append((functools.partial(forward, row, mid), b, b, mid))
    for row in range(nsup - 1, 0, -1):
        items.append((functools.partial(backward, row, row), where[("D", row, row)], where[("D", row, row)], row + 1))
        for low_row in range(row + 1, nsup):
            items.append(
                (functools.partial(backward, row, low_row), where[("L", low_row, row)], where[("D", row, row)], row + 1)
            )
    for low_row in range(1, nsup):
        b = where[("L", low_row, 0)]
        items.append((functools.partial(backward, 0, low_row), b, b, 1))

    for i in range(24 - tri(nsup)):
        share[tri(nsup) + i] = jnp.zeros(share.shape[1:], jnp.float32)
    for b in range(ahead):
        own(b)
    state = {"done": -1, "loaded": -1}
    seen = set()

    def fetch(i):
        if i <= state["loaded"] or i >= len(items) or items[i][2] + ahead > state["done"]:
            return
        b = items[i][1]
        if b not in seen:
            seen.add(b)
            arrived(b)
        blk_copy(b, i % 2).start()
        state["loaded"] = i

    todo, started, summed = 0, [], []
    ready_at = first0 - where[("L", 1, 0)] + nsup + 1
    finals = {}
    for i, (fn, b, avail, units) in enumerate(items):
        if fn.func is backward and fn.args[1] == nsup - 1:
            finals[i] = fn.args[0]
    for s in range(last + ahead):
        service(s)
        state["done"] = s
        if s == ready_at:
            begin()
        if s < ready_at:
            continue
        for row, since in list(summed):
            if s >= since + delay:
                reduce_second(row)
                summed.remove((row, since))
        for row, since in list(started):
            if s >= since + delay:
                reduce_first(row)
                started.remove((row, since))
                summed.append((row, s))
        budget = 10**6 if s >= last + ahead - 1 else pace if s >= sym0 + ahead else early
        while todo < len(items) and items[todo][2] + ahead <= s and budget > 0:
            fetch(todo)
            fetch(todo + 1)
            blk_copy(items[todo][1], todo % 2).wait()
            if todo == len(items) - nsup + 1:
                set_first(acc_g, 0, nsup - 1)
            items[todo][0](todo % 2)
            budget -= items[todo][3]
            if todo in finals:
                if finals[todo] == nsup - 1:
                    w_copy.wait_recv()
                finish_g(finals[todo])
                started.append((finals[todo], s))
            todo += 1
    rest = [row for row, since in started if row > 0]
    for row in rest:
        reduce_first(row)
    for row, since in summed:
        reduce_second(row)
    reduce_first(0)
    for row in rest:
        reduce_second(row)
    reduce_second(0)
    finish_low(0)
    finish_low(1)
    finish_mirror()
    finish_low(2)

    w_copy.wait_send()
    for g in range(3):
        for copy in low_copies(g):
            copy.wait_send()

    @pl.when(moves)
    def _():
        for row in range(1, nsup):
            mirror_copy(row).wait_send()

    for b in range(nb):
        z_copy(b, zh).wait_send()
        c_copy(b, 0, x, both, core).wait_send()
        if b in syms:
            for kind, row in out_right + out_left:
                dx_copy(b, kind, row, x, to_right).wait_send()
            dx_copy(b, 5, left, left, to_right, 0, part_size).wait_send()
            dx_copy(b, 6, right, right, to_left, part_size, part_size).wait_send()
            for kind, row, col, start, size in dc_kinds:
                dc_copy(b, kind, row, col, core, start, size).wait_send()
        elif b < last:
            x_copy(b, 0, x, both, to_right).wait_send()
            x_copy(b, 1, x, both, to_left).wait_send()
            x_copy(b, 2, left, half0, to_right).wait_send()
            x_copy(b, 3, right, half1, to_left).wait_send()
            for kind, col, parts in c_kinds[1:]:
                c_copy(b, kind, col, parts, core).wait_send()
    for row in range(nsup):
        for copy in first_stage(row) + second_stage(row):
            copy.wait_send()


def window_share(factor, dinv, tiles, weight, ncol):
    _, parts, nsup, _, rows, cols = factor.shape
    nb = tri(nsup)
    width, unit, pairs = 2 * rows, cols, tri(nsup)
    sems = pltpu.SemaphoreType.DMA
    f32, bf16 = jnp.float32, jnp.bfloat16
    return pl.pallas_call(
        functools.partial(window_kernel, nsup),
        out_shape=(
            jax.ShapeDtypeStruct((nb, parts, width, width), f32),
            jax.ShapeDtypeStruct((nsup, nsup, 16, cols), f32),
        ),
        in_specs=[
            pl.BlockSpec(memory_space=pl.ANY),
            pl.BlockSpec(memory_space=pl.ANY),
            pl.BlockSpec(memory_space=pltpu.SMEM),
            pl.BlockSpec(memory_space=pltpu.VMEM),
        ],
        out_specs=(pl.BlockSpec(memory_space=pl.ANY), pl.BlockSpec(memory_space=pltpu.VMEM)),
        scratch_shapes=[
            pltpu.VMEM((nb, parts, rows, cols), f32),
            pltpu.VMEM(weight.shape, f32),
            pltpu.VMEM((2, parts, width, width), f32),
            pltpu.VMEM((nsup, parts, width, cols), f32),
            pltpu.VMEM((2, tri(nsup - 1) * unit, width), f32),
            pltpu.VMEM((2, nsup * unit, width), f32),
            pltpu.VMEM((pairs * unit, width), bf16),
            pltpu.VMEM((pairs * unit, width), bf16),
            pltpu.VMEM((pairs * unit, width), bf16),
            pltpu.VMEM((pairs * unit, width), bf16),
            pltpu.VMEM((pairs, 2, 2, 16, width), f32),
            pltpu.VMEM((3, pairs, 2, 16, width // 2), f32),
            pltpu.VMEM((pairs, 2, 16, width // 2), f32),
            pltpu.VMEM((3, pairs, 16, cols), f32),
            pltpu.VMEM((24, 16, cols), f32),
            pltpu.VMEM((pairs, 16, cols), f32),
            pltpu.VMEM((3, cols, cols), f32),
            pltpu.VMEM((3, 8, 16, cols), f32),
            sems((nb,)), sems((nb,)), sems((4, nb)), sems((4, nb)), sems((5, nb)), sems((5, nb)),
            sems((2, nsup, 3)), sems((2, nsup, 3)), sems((nsup,)), sems((nsup,)), sems((3, 7)), sems((3, 7)), sems((2,)),
            *[sems((7, nsup - 1)) for _ in range(4)], sems((2,)), sems((nsup,)), sems((nb,)),
        ],
        compiler_params=pltpu.CompilerParams(
            collective_id=0, has_side_effects=True, vmem_limit_bytes=60 * 1024 * 1024
        ),
    )(factor, dinv, tiles, weight)[1]


def on_device(l_factor, dinv, weights, tiles):
    width = 2 * l_factor.shape[3]
    weight = jnp.broadcast_to(jnp.pad(weights[0], (0, 6))[:, None], (8, width))
    factor = jnp.swapaxes(l_factor, 3, 4)
    blocks = window_share(factor, dinv, tiles, weight, lax.axis_size("x"))
    return jnp.transpose(blocks, (0, 2, 1, 3))[:, None]


def solution(mesh):
    fine = Mesh(mesh.devices.reshape(2, 2, 2, 2, 2, 4), AXES)
    pole = ("a", "b", "zl", "core")
    return jax.shard_map(
        on_device,
        mesh=fine,
        in_specs=(P(pole, None, None, "zh", None, "x"), P(pole, None, None, "zh", "x"), P(pole, None), P()),
        out_specs=P(None, "zh", pole, None, "x"),
        check_vma=False,
    )
```
